128 devices in a mesh: node: 128 (over z, x, y, core).
Axes of the slice: x: 4, y: 4, z: 4, core: 2. Of those that a mesh axis runs over, the one named last changes fastest.
Arguments:
- labels: bfloat16 [524288, 512], P('node'), may hold values from -6 to 6
- seed_mask: int32 [524288], P('node'), may hold values 0 or 1
- band_w: bfloat16 [4096, 3, 128, 128], P('node'), may hold values from 0.0009994507 to 1
- far_block: int32 [128, 128, 2], P('node'), may hold values from 0 to 511
- far_tile: int32 [128, 128, 2], P('node'), may hold values from 0 to 31
- far_count: int32 [128, 128], P('node'), may hold values from 0 to 2, as said below
- far_w: bfloat16 [128, 128, 2, 8, 128], P('node'), may hold values from 0.049804688 to 2
Outputs:
- final_labels: bfloat16 [524288, 512], P('node')
- residual: float32 [2, 4096], P(None, 'node')
The draws below stay inside these ranges and needn't reach their ends.
Inputs may be any that keep to these rules, and one draw needn't show every extreme that they name: `far_count`: in every draw at least one destination shard has all 2 slots live from every source shard; other counts vary from pair to pair.
All inputs are finite; a program needn't handle non-finite values. No bound on the sum of `seed_mask` on one device may be relied on, other than what follows from the above.
Results may differ from the reference program's by a relative error of at most 0.0027.
Values may be sent and summed in bfloat16 or wider, within the bound.
A program may use at most 128 MiB of HBM per device.

```python
import math
import jax
import jax.numpy as jnp
from jax import lax

C = 512
NODE_DEV = 4096
TILE = 128
BLK = 8
SLOTS = 2
ITERS = 2
NODES = 524288
N_NODE = 128


def draw_far_count(key, part):
    first_key, second_key = jax.random.split(jax.random.fold_in(key, 17))
    counts = jax.random.randint(first_key, (N_NODE, N_NODE), 0, SLOTS + 1)
    busiest = jax.random.randint(second_key, (), 0, N_NODE)
    row_ids = jnp.arange(N_NODE)[:, None]
    return jnp.where(row_ids == busiest, SLOTS, counts).astype(jnp.int32)


def set_ends(values, rng, smallest, top_value):
    dims = values.shape
    place = [jax.random.randint(jax.random.fold_in(rng, axis), (), 0, dims[axis]) for axis in range(len(dims))]
    values = values.at[tuple(place)].set(smallest)
    longest = dims.index(max(dims))
    place[longest] = (place[longest] + 1) % dims[longest]
    return values.at[tuple(place)].set(top_value)


def block_scale(own_key, dims, cuts, smallest, high):
    factor_of, own = 1.0, jax.random.fold_in(own_key, 6)
    for dim, parts in cuts:
        steps = jnp.exp(jax.random.uniform(jax.random.fold_in(own, dim), (parts,), jnp.float32, smallest / len(cuts), high / len(cuts)))
        factor_of = factor_of * jnp.repeat(steps, dims[dim] // parts).reshape([-1 if axis == dim else 1 for axis in range(len(dims))])
    return factor_of


def normal_values(own_key, shape, width, most, pieces=(), dtype=jnp.bfloat16):
    array = width * jax.random.normal(own_key, shape, jnp.float32)
    if pieces:
        array = array * block_scale(own_key, shape, pieces, -0.22, 0.18)
    return jnp.clip(array, -most, most).astype(dtype)


def setup_inputs(seed: int = 0) -> dict:
    key_of = jax.random.split(jax.random.key(seed), 8)
    return {
        "labels": normal_values(key_of[0], (NODES, C), 1.0, 6.0, ((0, 128),)),
        "seed_mask": set_ends((jax.random.randint(key_of[1], (NODES,), 0, 4) < 1).astype(jnp.int32), jax.random.fold_in(key_of[1], 1), 0, 1),
        "band_w": jnp.clip(jnp.exp(math.log(1.0) - 6.9083047 * jax.random.uniform(key_of[2], (NODES // TILE, 3, TILE, TILE), jnp.float32) ** block_scale(key_of[2], (NODES // TILE, 3, TILE, TILE), ((0, 128),), -0.2, 0.2)), 0.0009994507, 1.0).astype(jnp.bfloat16),
        "far_block": set_ends(jax.random.randint(key_of[3], (N_NODE, N_NODE, SLOTS), 0, NODE_DEV // BLK), jax.random.fold_in(key_of[3], 1), 0, (NODE_DEV // BLK) - 1).astype(jnp.int32),
        "far_tile": set_ends(jax.random.randint(key_of[4], (N_NODE, N_NODE, SLOTS), 0, NODE_DEV // TILE), jax.random.fold_in(key_of[4], 1), 0, (NODE_DEV // TILE) - 1).astype(jnp.int32),
        "far_count": draw_far_count(jax.random.fold_in(key_of[7], 71), 0),
        "far_w": jnp.clip(jnp.exp(math.log(2.0) - 3.6927934 * jax.random.uniform(key_of[6], (N_NODE, N_NODE, SLOTS, BLK, TILE), jnp.float32) ** block_scale(key_of[6], (N_NODE, N_NODE, SLOTS, BLK, TILE), ((0, 128),), -0.2, 0.2)), 0.049804688, 2.0).astype(jnp.bfloat16),
    }


def live_table(count_row):
    return (jnp.arange(SLOTS)[None, :] < count_row[:, None]).astype(jnp.float32)

def reference(labels, seed_mask, band_w, far_block, far_tile, far_count, far_w):
    tile_total = labels.shape[0] // TILE
    block_count = NODE_DEV // BLK
    band_wide = band_w.astype(jnp.float32)
    degree_band = lax.optimization_barrier(jnp.sum(band_wide, axis=(1, 3)))

    def far_degree(packed):
        tiles_here, count_here, weight_here = packed
        live_weights = weight_here.astype(jnp.float32) * live_table(count_here)[:, :, None, None]
        weight_sums = lax.optimization_barrier(jnp.sum(live_weights, axis=2)).reshape(-1, TILE)
        return jnp.zeros((NODE_DEV // TILE, TILE), jnp.float32).at[tiles_here.reshape(-1)].add(weight_sums)
    degree_far = lax.map(far_degree, (far_tile, far_count, far_w)).reshape(tile_total, TILE)
    degree = degree_band + degree_far
    seeded = (seed_mask == 1).reshape(tile_total, TILE, 1)
    clamped = labels.astype(jnp.float32).reshape(tile_total, TILE, C)
    current = labels
    residuals = []
    for sweep in range(ITERS):
        tiles = current.astype(jnp.float32).reshape(tile_total, TILE, C)
        band_sum = jnp.zeros((tile_total, TILE, C), jnp.float32)
        for offset in (-1, 0, 1):
            source = jnp.roll(tiles, -offset, axis=0)
            band_sum = band_sum + jnp.einsum('itr,irc->itc', band_wide[:, offset + 1], source)
        blocks_all = current.reshape(N_NODE, block_count, BLK, C)

        def far_part(packed):
            wanted, tiles_here, count_here, weight_here = packed
            blocks = blocks_all[jnp.arange(N_NODE)[:, None], wanted].astype(jnp.float32)
            live_weights = weight_here.astype(jnp.float32) * live_table(count_here)[:, :, None, None]
            contrib = jnp.einsum('skqt,skqc->sktc', live_weights, blocks)
            return jnp.zeros((NODE_DEV // TILE, TILE, C), jnp.float32).at[tiles_here.reshape(-1)].add(contrib.reshape(-1, TILE, C))
        far_sum = lax.map(far_part, (far_block, far_tile, far_count, far_w)).reshape(tile_total, TILE, C)
        averaged = (band_sum + far_sum) / degree[:, :, None]
        row_scale = jnp.sqrt(lax.optimization_barrier(jnp.mean(averaged * averaged, axis=2, keepdims=True)))
        scaled = averaged / jnp.maximum(row_scale, 0.05)
        fresh = jnp.where(seeded, clamped, scaled).astype(jnp.bfloat16)
        residuals.append(lax.optimization_barrier(jnp.sum(jnp.abs(fresh.astype(jnp.float32) - tiles), axis=(1, 2))))
        current = fresh.reshape(labels.shape[0], C)
    return (current, jnp.stack(residuals))
```

```python
import functools

import jax
import jax.numpy as jnp
from jax import lax
from jax.experimental import pallas as pl
from jax.experimental.pallas import tpu as pltpu
from jax.sharding import PartitionSpec as P

MESH = pl.DeviceIdType.MESH
BF = jnp.bfloat16
F32 = jnp.float32
STEP = 37
CHUNK = 16
LAG = 8


def rows_of(start, size):
    return pl.ds(pl.multiple_of(start, size), size)


def kernel(
    n, tiles, tile, classes, slots, blk,
    lab_hbm, bw_hbm, fw_hbm, fb_hbm, ft_hbm, fc_hbm, sm_hbm,
    out_hbm, res_ref,
    p0, p1, g32, acc, halo, send, recv, bw, fw, wp, wt, oh, dt, inv, outb, resb,
    fb, ft, fc, sm, req, qv, qs,
    load_sem, small_sem, req_ssem, req_rsem, q_sem, ssem, rsem, h_ssem, h_rsem, o_sem,
):
    me = lax.axis_index("node")
    nodes = tiles * tile
    pair = slots * blk
    wide = n * pair
    chunks = n // CHUNK
    kdim = CHUNK * pair

    def shift(p):
        return lax.rem(p * STEP, n)

    def source_of(p):
        return lax.rem(me + shift(p), n)

    def target_of(p):
        return lax.rem(me - shift(p) + n, n)

    barrier = pltpu.get_barrier_semaphore()

    def greet(i, carry):
        pl.semaphore_signal(barrier, inc=1, device_id=(lax.rem(me + i, n),), device_id_type=MESH)
        return carry

    lax.fori_loop(1, n, greet, 0)

    small = [
        pltpu.make_async_copy(src, dst, small_sem.at[i])
        for i, (src, dst) in enumerate(((fb_hbm, fb), (ft_hbm, ft), (fc_hbm, fc), (sm_hbm, sm)))
    ]
    large = [
        pltpu.make_async_copy(fw_hbm, fw, load_sem.at[0]),
        pltpu.make_async_copy(lab_hbm, p0.at[pl.ds(tile, nodes)], load_sem.at[1]),
        pltpu.make_async_copy(bw_hbm, bw, load_sem.at[2]),
    ]
    for copy in small + large:
        copy.start()
    for copy in small:
        copy.wait()

    lane = lax.broadcasted_iota(jnp.int32, (n, tile), 1)
    columns = [jnp.broadcast_to(fb[k : k + 1, :], (n, n)).T for k in range(slots)]
    table = jnp.where(lane == 0, columns[0], columns[1])
    for s in range(n):
        req[s] = table[s : s + 1]

    pl.semaphore_wait(barrier, n - 1)

    def ask(p, carry):
        s = source_of(p)
        pltpu.make_async_remote_copy(
            req.at[s], qv.at[p], req_ssem, req_rsem, device_id=(s,), device_id_type=MESH
        ).start()
        return carry

    lax.fori_loop(1, n, ask, 0)
    qv[0] = req[me]
    large[1].wait()

    nxt = lax.rem(me + 1, n)
    prv = lax.rem(me + n - 1, n)

    def halo_copies(it, cur):
        up = pltpu.make_async_remote_copy(
            cur.at[pl.ds(nodes, tile)], halo.at[it, 0], h_ssem.at[it, 0], h_rsem.at[it, 0],
            device_id=(nxt,), device_id_type=MESH,
        )
        down = pltpu.make_async_remote_copy(
            cur.at[pl.ds(tile, tile)], halo.at[it, 1], h_ssem.at[it, 1], h_rsem.at[it, 1],
            device_id=(prv,), device_id_type=MESH,
        )
        return up, down

    halo0 = halo_copies(0, p0)
    for copy in halo0:
        copy.start()

    def widen(t, carry):
        rows = p0[rows_of(tile + t * tile, tile), :].astype(F32)
        g32[rows_of(t * (tile // blk), tile // blk)] = rows.reshape(tile // blk, blk, classes)
        return carry

    lax.fori_loop(0, tiles, widen, 0)

    large[0].wait()

    def place(p, carry):
        wp[p] = fw[source_of(p)]
        return carry

    lax.fori_loop(0, n, place, 0)

    def turn(j, carry):
        part = wp[pl.ds(j * (tile // pair), tile // pair)].reshape(tile, tile)
        wt[:, rows_of(j * tile, tile)] = part.astype(F32).T.astype(BF)
        return carry

    lax.fori_loop(0, wide // tile, turn, 0)

    row8 = lax.broadcasted_iota(jnp.int32, (8, n), 0)
    number = [jnp.where(fc[...] > k, ft[k : k + 1, :], -1) for k in range(slots)]
    numbers = jnp.where(row8 == 0, number[0], number[1]).astype(F32).astype(BF)
    step = 512

    def mark(j, carry):
        col = lax.broadcasted_iota(jnp.int32, (n, step), 1) + j * step
        src = lax.rem(me + lax.rem((col // pair) * STEP, n), n)
        pick = jnp.where(lax.broadcasted_iota(jnp.int32, (n, step), 0) == src, 1.0, 0.0).astype(BF)
        found = jnp.dot(numbers, pick, preferred_element_type=F32)
        first = lax.rem(col[:1] // blk, slots) == 0
        mine = jnp.where(first, found[:1], found[1:2])
        ids = lax.broadcasted_iota(jnp.int32, (tiles, step), 0).astype(F32)
        oh[:, rows_of(j * step, step)] = jnp.where(mine == ids, 1.0, 0.0)
        return carry

    lax.fori_loop(0, wide // step, mark, 0)

    far_deg = jnp.dot(oh[...].astype(BF), wp[...].reshape(wide, tile), preferred_element_type=F32)
    seeds = sm[...].astype(F32)
    stack = jnp.concatenate([far_deg, seeds, jnp.zeros((tile - 2 * tiles, tile), F32)], axis=0)
    dt[...] = stack.T
    large[2].wait()

    def invert(t, carry):
        both = dt[...]
        far = jnp.sum(jnp.where(lane == t, both, 0.0), axis=1, keepdims=True)
        seed = jnp.sum(jnp.where(lane == t + tiles, both, 0.0), axis=1, keepdims=True)
        band = bw[t, 0].astype(F32) + bw[t, 1].astype(F32) + bw[t, 2].astype(F32)
        one = 1.0 / (jnp.sum(band, axis=1, keepdims=True) + far)
        inv[rows_of(t * tile, tile), :] = jnp.broadcast_to(jnp.where(seed > 0.5, -one, one), (tile, tile))
        return carry

    lax.fori_loop(0, tiles, invert, 0)

    asked = pltpu.make_async_remote_copy(
        req.at[pl.ds(1, n - 1)], qv.at[pl.ds(1, n - 1)], req_ssem, req_rsem,
        device_id=(nxt,), device_id_type=MESH,
    )
    asked.wait_recv()
    to_scalar = pltpu.make_async_copy(qv, qs, q_sem)
    to_scalar.start()
    to_scalar.wait()

    def exchange(it):
        def gather(p):
            blocks = [g32[qs[p, 0, k]] for k in range(slots)]
            return jnp.concatenate(blocks, axis=0).astype(BF)

        def ship(p):
            pltpu.make_async_remote_copy(
                send.at[it, p], recv.at[it, p], ssem.at[it], rsem.at[it, p // CHUNK],
                device_id=(target_of(p),), device_id_type=MESH,
            ).start()

        recv[it, 0] = gather(0)

        def first(p, carry):
            send[it, p] = gather(p)
            return carry

        lax.fori_loop(1, 1 + LAG, first, 0)

        def both(p, carry):
            send[it, p + LAG] = gather(p + LAG)
            ship(p)
            return carry

        lax.fori_loop(1, n - LAG, both, 0)

        def last(p, carry):
            ship(p)
            return carry

        lax.fori_loop(n - LAG, n, last, 0)

    def band(cur, t):
        lhs = jnp.concatenate([bw[t, 0], bw[t, 1], bw[t, 2]], axis=1)
        rhs = cur[pl.ds(pl.multiple_of(t * tile, tile), 3 * tile), :]
        acc[rows_of(t * tile, tile), :] = jnp.dot(lhs, rhs, preferred_element_type=F32)

    def band_all(it, cur, copies):
        def inner(t, carry):
            band(cur, t)
            return carry

        lax.fori_loop(1, tiles - 1, inner, 0)
        for copy in copies:
            copy.wait_recv()
        cur[pl.ds(0, tile), :] = halo[it, 0]
        cur[pl.ds(tile + nodes, tile), :] = halo[it, 1]
        band(cur, 0)
        band(cur, tiles - 1)

    group = 4

    def far(it):
        for c in range(chunks):
            low = 1 if c == 0 else 0
            span = pl.ds(c * CHUNK + low, CHUNK - low)
            pltpu.make_async_remote_copy(
                send.at[it, span], recv.at[it, span], ssem.at[it], rsem.at[it, c],
                device_id=(nxt,), device_id_type=MESH,
            ).wait_recv()

        def chunk(c, carry):
            rhs = recv[it, pl.ds(c * CHUNK, CHUNK)].reshape(kdim, classes)
            cols = rows_of(c * kdim, kdim)

            def some(g, inner):
                weights = wt[:, cols]
                parts = []
                for j in range(group):
                    keep = oh[pl.ds(g * group + j, 1), cols].astype(BF)
                    parts.append(weights * jnp.broadcast_to(keep, (tile, kdim)))
                lhs = jnp.concatenate(parts, axis=0)
                rows = rows_of(g * group * tile, group * tile)
                acc[rows, :] = acc[rows, :] + jnp.dot(lhs, rhs, preferred_element_type=F32)
                return inner

            lax.fori_loop(0, tiles // group, some, 0)
            return carry

        lax.fori_loop(0, chunks, chunk, 0)

    sub = 32

    def fresh(row):
        spread = acc[rows_of(row, sub), :]
        signed = inv[rows_of(row, sub), :]
        one = jnp.abs(signed)
        square = jnp.sum(spread * spread, axis=1, keepdims=True)
        mean = square * one * one * (1.0 / classes)
        factor = one / jnp.maximum(jnp.sqrt(mean), 0.05)
        reps = classes // tile
        scaled = spread * jnp.concatenate([factor] * reps, axis=1)
        seeded = jnp.concatenate([signed] * reps, axis=1) < 0.0
        given = p0[pl.ds(pl.multiple_of(tile + row, sub), sub), :].astype(F32)
        return jnp.where(seeded, given, scaled).astype(BF)

    def fold(change):
        total = jnp.sum(change, axis=0, keepdims=True)
        return sum(total[:, i * tile : (i + 1) * tile] for i in range(classes // tile))

    exchange(0)
    band_all(0, p0, halo0)
    far(0)

    def finish0(i, carry):
        row = i * sub
        new = fresh(row)
        p1[pl.ds(pl.multiple_of(tile + row, sub), sub), :] = new
        g32[pl.ds(i * (sub // blk), sub // blk)] = new.astype(F32).reshape(sub // blk, blk, classes)
        return carry

    lax.fori_loop(0, nodes // sub, finish0, 0)

    halo1 = halo_copies(1, p1)
    for copy in halo1:
        copy.start()
    exchange(1)

    def change0(t, carry):
        total = jnp.zeros((1, tile), F32)
        for j in range(tile // sub):
            rows = pl.ds(pl.multiple_of(tile + t * tile + j * sub, sub), sub)
            total = total + fold(jnp.abs(p1[rows, :].astype(F32) - p0[rows, :].astype(F32)))
        resb[0, pl.ds(t, 1), :] = total
        return carry

    lax.fori_loop(0, tiles, change0, 0)
    band_all(1, p1, halo1)
    far(1)

    def out_copy(t):
        rows = rows_of(t * tile, tile)
        return pltpu.make_async_copy(outb.at[rows], out_hbm.at[rows], o_sem)

    def finish1(t, carry):
        total = jnp.zeros((1, tile), F32)
        for j in range(tile // sub):
            row = t * tile + j * sub
            new = fresh(row)
            outb[rows_of(row, sub), :] = new
            old = p1[pl.ds(pl.multiple_of(tile + row, sub), sub), :].astype(F32)
            total = total + fold(jnp.abs(new.astype(F32) - old))
        resb[1, pl.ds(t, 1), :] = total

        @pl.when(t > 0)
        def _():
            out_copy(t - 1).start()

        return carry

    lax.fori_loop(0, tiles, finish1, 0)
    out_copy(tiles - 1).start()

    for it in range(2):
        block = jnp.concatenate([resb[it], jnp.zeros((tile - tiles, tile), F32)], axis=0)
        res_ref[it : it + 1, :] = jnp.sum(block.T, axis=0, keepdims=True)[:, :tiles]

    asked.wait_send()
    for copy in halo0 + halo1:
        copy.wait_send()
    for it in range(2):
        span = pl.ds(1, n - 1)
        pltpu.make_async_remote_copy(
            send.at[it, span], recv.at[it, span], ssem.at[it], rsem.at[it, 0],
            device_id=(nxt,), device_id_type=MESH,
        ).wait_send()
    pltpu.make_async_copy(outb, out_hbm, o_sem).wait()


def body(labels, seed_mask, band_w, far_block, far_tile, far_count, far_w):
    nodes, classes = labels.shape
    tiles, _, tile, _ = band_w.shape
    _, n, slots, blk, _ = far_w.shape
    any_space = pl.BlockSpec(memory_space=pl.ANY)
    vmem = pl.BlockSpec(memory_space=pltpu.VMEM)
    dma = pltpu.SemaphoreType.DMA
    wide = n * slots * blk
    final, residual = pl.pallas_call(
        functools.partial(kernel, n, tiles, tile, classes, slots, blk),
        out_shape=(
            jax.ShapeDtypeStruct((nodes, classes), BF),
            jax.ShapeDtypeStruct((2, tiles), F32),
        ),
        in_specs=[any_space] * 7,
        out_specs=(any_space, vmem),
        scratch_shapes=[
            pltpu.VMEM((nodes + 2 * tile, classes), BF),
            pltpu.VMEM((nodes + 2 * tile, classes), BF),
            pltpu.VMEM((nodes // blk, blk, classes), F32),
            pltpu.VMEM((nodes, classes), F32),
            pltpu.VMEM((2, 2, tile, classes), BF),
            pltpu.VMEM((2, n, slots * blk, classes), BF),
            pltpu.VMEM((2, n, slots * blk, classes), BF),
            pltpu.VMEM(band_w.shape, BF),
            pltpu.VMEM((n, slots * blk, tile), BF),
            pltpu.VMEM((n, slots * blk, tile), BF),
            pltpu.VMEM((tile, wide), BF),
            pltpu.VMEM((tiles, wide), F32),
            pltpu.VMEM((tile, tile), F32),
            pltpu.VMEM((nodes, tile), F32),
            pltpu.VMEM((nodes, classes), BF),
            pltpu.VMEM((2, tiles, tile), F32),
            pltpu.VMEM((slots, n), jnp.int32),
            pltpu.VMEM((slots, n), jnp.int32),
            pltpu.VMEM((1, n), jnp.int32),
            pltpu.VMEM((tiles, tile), jnp.int32),
            pltpu.VMEM((n, 1, tile), jnp.int32),
            pltpu.VMEM((n, 1, tile), jnp.int32),
            pltpu.SMEM((n, 1, tile), jnp.int32),
            dma((3,)),
            dma((4,)),
            dma,
            dma,
            dma,
            dma((2,)),
            dma((2, n // CHUNK)),
            dma((2, 2)),
            dma((2, 2)),
            dma,
        ],
        compiler_params=pltpu.CompilerParams(
            collective_id=0, has_side_effects=True, vmem_limit_bytes=62 * 2**20
        ),
    )(
        labels,
        band_w,
        far_w.reshape(n, slots * blk, tile),
        far_block[0].T,
        far_tile[0].T,
        far_count,
        seed_mask.reshape(tiles, tile),
    )
    return final, residual


def solution(mesh):
    placed = (
        P("node", None),
        P("node"),
        P("node", None, None, None),
        P("node", None, None),
        P("node", None, None),
        P("node", None),
        P("node", None, None, None, None),
    )
    return jax.shard_map(
        body,
        mesh=mesh,
        in_specs=placed,
        out_specs=(P("node", None), P(None, "node")),
        check_vma=False,
    )
```

```python
import functools

import jax
import jax.numpy as jnp
from jax import lax
from jax.experimental import pallas as pl
from jax.experimental.pallas import tpu as pltpu
from jax.sharding import PartitionSpec as P

MESH = pl.DeviceIdType.MESH
BF = jnp.bfloat16
F32 = jnp.float32
STEP = 91
BACK = 83
CUTS = (0, 32, 64, 88, 112, 128)
RUN = 8


def rows_of(start, size):
    return pl.ds(pl.multiple_of(start, size), size)


def kernel(
    n, tiles, tile, classes, slots, blk,
    lab_hbm, bw_hbm, fw_hbm, fb_hbm, ft_hbm, fc_hbm, sm_hbm,
    out_ref, res_ref,
    p0, p1, g32, acc, halo, send, recv, bw, fw, wp, wt, oh, dt, inv, resb, sum0, sum1, fac0, fac1,
    fb, ft, fc, sm, req, qv, qs,
    load_sem, small_sem, req_ssem, req_rsem, q_sem, ssem, rsem, h_ssem, h_rsem,
):
    me = lax.axis_index("node")
    nodes = tiles * tile
    pair = slots * blk
    wide = n * pair
    sums, factors = (sum0, sum1), (fac0, fac1)
    chunks = len(CUTS) - 1

    def plus(a, b):
        return (a + b) & (n - 1)

    def source_of(p):
        return plus(me, p * STEP)

    def target_of(p):
        return plus(me, -p * STEP)

    def far_first(i):
        return i ^ 84

    def each_peer(step):
        lax.fori_loop(0, 84, step, 0)
        lax.fori_loop(85, n, step, 0)

    small = [
        pltpu.make_async_copy(src, dst, small_sem.at[i])
        for i, (src, dst) in enumerate(((fb_hbm, fb), (ft_hbm, ft), (fc_hbm, fc), (sm_hbm, sm)))
    ]
    large = [
        pltpu.make_async_copy(fw_hbm, fw, load_sem.at[0]),
        pltpu.make_async_copy(lab_hbm, p0.at[pl.ds(tile, nodes)], load_sem.at[1]),
        pltpu.make_async_copy(bw_hbm, bw, load_sem.at[2]),
    ]
    for copy in small + large:
        copy.start()
    barrier = pltpu.get_barrier_semaphore()

    def greet(i, carry):
        pl.semaphore_signal(
            barrier, inc=1, device_id=(plus(me, far_first(i)),), device_id_type=MESH
        )
        return carry

    with jax.named_scope("s_greet"):
        each_peer(greet)
    for copy in small:
        copy.wait()

    lane = lax.broadcasted_iota(jnp.int32, (n, tile), 1)
    columns = [jnp.broadcast_to(fb[k : k + 1, :], (n, n)).T for k in range(slots)]
    table = jnp.where(lane == 0, columns[0], columns[1])
    for s in range(n):
        req[s] = table[s : s + 1]

    with jax.named_scope("s_barrier"):
        pl.semaphore_wait(barrier, n - 1)

    def ask(i, carry):
        distance = far_first(i)
        s = plus(me, distance)
        pltpu.make_async_remote_copy(
            req.at[s], qv.at[(distance * BACK) & (n - 1)], req_ssem, req_rsem,
            device_id=(s,), device_id_type=MESH,
        ).start()
        return carry

    with jax.named_scope("s_ask"):
        each_peer(ask)
    qv[0] = req[me]
    large[1].wait()

    nxt = plus(me, 1)
    prv = plus(me, n - 1)

    def halo_copies(it, cur):
        up = pltpu.make_async_remote_copy(
            cur.at[pl.ds(nodes, tile)], halo.at[it, 0], h_ssem.at[it, 0], h_rsem.at[it, 0],
            device_id=(nxt,), device_id_type=MESH,
        )
        down = pltpu.make_async_remote_copy(
            cur.at[pl.ds(tile, tile)], halo.at[it, 1], h_ssem.at[it, 1], h_rsem.at[it, 1],
            device_id=(prv,), device_id_type=MESH,
        )
        return up, down

    halo0 = halo_copies(0, p0)
    for copy in halo0:
        copy.start()

    def widen(t, carry):
        rows = p0[rows_of(tile + t * tile, tile), :].astype(F32)
        g32[rows_of(t * (tile // blk), tile // blk)] = rows.reshape(tile // blk, blk, classes)
        return carry

    lax.fori_loop(0, tiles, widen, 0)
    edge = jnp.zeros((tile, classes), BF)
    for ref in (p0, p1):
        ref[pl.ds(0, tile), :] = edge
        ref[pl.ds(tile + nodes, tile), :] = edge

    large[0].wait()

    def place(p, carry):
        wp[p] = fw[source_of(p)]
        return carry

    lax.fori_loop(0, n, place, 0)

    def turn(j, carry):
        part = wp[pl.ds(j * (tile // pair), tile // pair)].reshape(tile, tile)
        wt[:, rows_of(j * tile, tile)] = part.astype(F32).T.astype(BF)
        return carry

    lax.fori_loop(0, wide // tile, turn, 0)

    row8 = lax.broadcasted_iota(jnp.int32, (8, n), 0)
    number = [jnp.where(fc[...] > k, ft[k : k + 1, :], -1) for k in range(slots)]
    numbers = jnp.where(row8 == 0, number[0], number[1]).astype(F32).astype(BF)
    step = 512

    def mark(j, carry):
        col = lax.broadcasted_iota(jnp.int32, (n, step), 1) + j * step
        src = (me + (col // pair) * STEP) & (n - 1)
        pick = jnp.where(lax.broadcasted_iota(jnp.int32, (n, step), 0) == src, 1.0, 0.0).astype(BF)
        found = jnp.dot(numbers, pick, preferred_element_type=F32)
        first = lax.rem(col[:1] // blk, slots) == 0
        mine = jnp.where(first, found[:1], found[1:2])
        ids = lax.broadcasted_iota(jnp.int32, (tiles, step), 0).astype(F32)
        oh[:, rows_of(j * step, step)] = jnp.where(mine == ids, 1.0, 0.0)
        return carry

    lax.fori_loop(0, wide // step, mark, 0)

    far_deg = jnp.dot(oh[...].astype(BF), wp[...].reshape(wide, tile), preferred_element_type=F32)
    seeds = sm[...].astype(F32)
    stack = jnp.concatenate([far_deg, seeds, jnp.zeros((tile - 2 * tiles, tile), F32)], axis=0)
    dt[...] = stack.T
    large[2].wait()

    def invert(i, carry):
        both = dt[...]
        for k in range(4):
            t = i * 4 + k
            far = jnp.sum(jnp.where(lane == t, both, 0.0), axis=1, keepdims=True)
            seed = jnp.sum(jnp.where(lane == t + tiles, both, 0.0), axis=1, keepdims=True)
            weight = bw[t, 0].astype(F32) + bw[t, 1].astype(F32) + bw[t, 2].astype(F32)
            one = 1.0 / (jnp.sum(weight, axis=1, keepdims=True) + far)
            inv[rows_of(t * tile, tile), :] = jnp.broadcast_to(jnp.where(seed > 0.5, -one, one), (tile, tile))
        return carry

    with jax.named_scope("s_invert"):
        lax.fori_loop(0, tiles // 4, invert, 0)

    asked = pltpu.make_async_remote_copy(
        req.at[pl.ds(1, n - 1)], qv.at[pl.ds(1, n - 1)], req_ssem, req_rsem,
        device_id=(nxt,), device_id_type=MESH,
    )
    with jax.named_scope("s_waitreq"):
        asked.wait_recv()
    def to_scalar(g):
        span = pl.ds(g * RUN, RUN)
        return pltpu.make_async_copy(qv.at[span], qs.at[span], q_sem.at[g])

    runs = n // RUN
    for g in range(runs):
        to_scalar(g).start()

    def exchange(it):
        def gather(p):
            blocks = [g32[qs[p, 0, k]] for k in range(slots)]
            return jnp.concatenate(blocks, axis=0).astype(BF)

        def load(g, low=0):
            if it == 0:
                to_scalar(g).wait()
            for j in range(low, RUN):
                send[it, g * RUN + j] = gather(g * RUN + j)

        def ship(g, low=0):
            c = sum((g >= cut // RUN).astype(jnp.int32) for cut in CUTS[1:-1])
            for j in range(low, RUN):
                p = g * RUN + j
                pltpu.make_async_remote_copy(
                    send.at[it, p], recv.at[it, p], ssem.at[it], rsem.at[it, c],
                    device_id=(target_of(p),), device_id_type=MESH,
                ).start()

        def both(g, carry):
            load(g)
            ship(g - 1)
            return carry

        zero = jnp.int32(0)
        load(zero, 1)
        recv[it, 0] = gather(0)
        load(zero + 1)
        ship(zero, 1)
        lax.fori_loop(2, runs, both, 0)
        ship(zero + (runs - 1))

    def band(cur, t):
        lhs = jnp.concatenate([bw[t, 0], bw[t, 1], bw[t, 2]], axis=1)
        rhs = cur[pl.ds(pl.multiple_of(t * tile, tile), 3 * tile), :]
        acc[rows_of(t * tile, tile), :] = jnp.dot(lhs, rhs, preferred_element_type=F32)

    def band_all(cur):
        def inner(i, carry):
            band(cur, 2 * i)
            band(cur, 2 * i + 1)
            return carry

        lax.fori_loop(0, tiles // 2, inner, 0)

    def edges(it, copies):
        for copy in copies:
            copy.wait_recv()
        for side, t, o in ((0, 0, 0), (1, tiles - 1, 2)):
            rows = pl.ds(t * tile, tile)
            acc[rows, :] = acc[rows, :] + jnp.dot(bw[t, o], halo[it, side], preferred_element_type=F32)

    def arrived(it, c):
        low, high = max(CUTS[c], 1), CUTS[c + 1]
        span = pl.ds(low, high - low)
        pltpu.make_async_remote_copy(
            send.at[it, span], recv.at[it, span], ssem.at[it], rsem.at[it, c],
            device_id=(nxt,), device_id_type=MESH,
        ).wait_recv()

    def product(it, c, t, count):
        low, size = CUTS[c], CUTS[c + 1] - CUTS[c]
        cols = pl.ds(low * pair, size * pair)
        rhs = recv[it, pl.ds(low, size)].reshape(size * pair, classes)
        weights = wt[:, cols]
        parts = []
        for j in range(count):
            keep = oh[pl.ds(t + j, 1), cols].astype(BF)
            parts.append(weights * jnp.broadcast_to(keep, (tile, size * pair)))
        lhs = jnp.concatenate(parts, axis=0)
        return jnp.dot(lhs, rhs, preferred_element_type=F32)

    group = 4

    def far(it, copies):
        for c in range(chunks - 1):
            with jax.named_scope(f"s_wait{c}"):
                arrived(it, c)

            def some(g, carry, c=c):
                rows = rows_of(g * group * tile, group * tile)
                acc[rows, :] = acc[rows, :] + product(it, c, g * group, group)
                return carry

            with jax.named_scope(f"s_mm{c}"):
                lax.fori_loop(0, tiles // group, some, 0)
        edges(it, copies)
        with jax.named_scope("s_waitlast"):
            arrived(it, chunks - 1)

    sub = 32
    reps = classes // tile

    def scale(it, t, slot):
        spread = acc[rows_of(t * tile, tile), :] + product(it, chunks - 1, t, 1)
        sums[slot][...] = spread
        one = jnp.abs(inv[rows_of(t * tile, tile), :])
        square = jnp.sum(spread * spread, axis=1, keepdims=True)
        mean = square * one * one * (1.0 / classes)
        factors[slot][...] = one / jnp.maximum(jnp.sqrt(mean), 0.05)

    def fresh(t, slot, j):
        part = pl.ds(j * sub, sub)
        row = t * tile + j * sub
        scaled = sums[slot][part, :] * jnp.concatenate([factors[slot][part, :]] * reps, axis=1)
        seeded = jnp.concatenate([inv[rows_of(row, sub), :]] * reps, axis=1) < 0.0
        given = p0[pl.ds(pl.multiple_of(tile + row, sub), sub), :].astype(F32)
        return jnp.where(seeded, given, scaled)

    def fold(change):
        total = jnp.sum(change.reshape(sub // 8, 8, classes), axis=0)
        return sum(total[:, i * tile : (i + 1) * tile] for i in range(reps))

    def finish(it, write):
        def step(i, carry):
            t = 2 * i
            scale(it, t + 1, 1)
            write(t, 0)
            scale(it, t + 2, 0)
            write(t + 1, 1)
            return carry

        last = jnp.int32(tiles - 1)
        scale(it, jnp.int32(0), 0)
        lax.fori_loop(0, tiles // 2 - 1, step, 0)
        scale(it, last, 1)
        write(last - 1, 0)
        write(last, 1)

    with jax.named_scope("s_exchange0"):
        exchange(0)
    with jax.named_scope("s_band0"):
        band_all(p0)
    far(0, halo0)

    def write0(t, slot):
        for j in range(tile // sub):
            new = fresh(t, slot, j)
            g32[pl.ds(t * (tile // blk) + j * (sub // blk), sub // blk)] = new.reshape(sub // blk, blk, classes)
            p1[pl.ds(pl.multiple_of(tile + t * tile + j * sub, sub), sub), :] = new.astype(BF)

    with jax.named_scope("s_finish0"):
        finish(0, write0)

    halo1 = halo_copies(1, p1)
    for copy in halo1:
        copy.start()
    with jax.named_scope("s_exchange1"):
        exchange(1)

    def change0(t, carry):
        total = jnp.zeros((8, tile), F32)
        for j in range(tile // sub):
            rows = pl.ds(pl.multiple_of(tile + t * tile + j * sub, sub), sub)
            total = total + fold(jnp.abs(p1[rows, :].astype(F32) - p0[rows, :].astype(F32)))
        resb[0, t] = total
        return carry

    with jax.named_scope("s_change0"):
        lax.fori_loop(0, tiles, change0, 0)
    with jax.named_scope("s_band1"):
        band_all(p1)
    far(1, halo1)

    def write1(t, slot):
        total = jnp.zeros((8, tile), F32)
        for j in range(tile // sub):
            row = t * tile + j * sub
            new = fresh(t, slot, j).astype(BF)
            out_ref[rows_of(row, sub), :] = new
            old = p1[pl.ds(pl.multiple_of(tile + row, sub), sub), :].astype(F32)
            total = total + fold(jnp.abs(new.astype(F32) - old))
        resb[1, t] = total

    with jax.named_scope("s_finish1"):
        finish(1, write1)

    with jax.named_scope("s_res"):
        for it in range(2):
            block = jnp.concatenate([jnp.sum(resb[it], axis=1), jnp.zeros((tile - tiles, tile), F32)], axis=0)
            res_ref[it : it + 1, :] = jnp.sum(block.T, axis=0, keepdims=True)[:, :tiles]

    asked.wait_send()
    for copy in halo0 + halo1:
        copy.wait_send()
    for it in range(2):
        span = pl.ds(1, n - 1)
        pltpu.make_async_remote_copy(
            send.at[it, span], recv.at[it, span], ssem.at[it], rsem.at[it, 0],
            device_id=(nxt,), device_id_type=MESH,
        ).wait_send()


def body(labels, seed_mask, band_w, far_block, far_tile, far_count, far_w):
    nodes, classes = labels.shape
    tiles, _, tile, _ = band_w.shape
    _, n, slots, blk, _ = far_w.shape
    hbm = pl.BlockSpec(memory_space=pltpu.HBM)
    vmem = pl.BlockSpec(memory_space=pltpu.VMEM)
    dma = pltpu.SemaphoreType.DMA
    wide = n * slots * blk
    final, residual = pl.pallas_call(
        functools.partial(kernel, n, tiles, tile, classes, slots, blk),
        out_shape=(
            pltpu.VMEM((nodes, classes), BF),
            pltpu.VMEM((2, tiles), F32),
        ),
        in_specs=[hbm] * 7,
        out_specs=(vmem, vmem),
        scratch_shapes=[
            pltpu.VMEM((nodes + 2 * tile, classes), BF),
            pltpu.VMEM((nodes + 2 * tile, classes), BF),
            pltpu.VMEM((nodes // blk, blk, classes), F32),
            pltpu.VMEM((nodes, classes), F32),
            pltpu.VMEM((2, 2, tile, classes), BF),
            pltpu.VMEM((2, n, slots * blk, classes), BF),
            pltpu.VMEM((2, n, slots * blk, classes), BF),
            pltpu.VMEM(band_w.shape, BF),
            pltpu.VMEM((n, slots * blk, tile), BF),
            pltpu.VMEM((n, slots * blk, tile), BF),
            pltpu.VMEM((tile, wide), BF),
            pltpu.VMEM((tiles, wide), F32),
            pltpu.VMEM((tile, tile), F32),
            pltpu.VMEM((nodes, tile), F32),
                pltpu.VMEM((2, tiles, 8, tile), F32),
            pltpu.VMEM((tile, classes), F32),
            pltpu.VMEM((tile, classes), F32),
            pltpu.VMEM((tile, tile), F32),
            pltpu.VMEM((tile, tile), F32),
            pltpu.VMEM((slots, n), jnp.int32),
            pltpu.VMEM((slots, n), jnp.int32),
            pltpu.VMEM((1, n), jnp.int32),
            pltpu.VMEM((tiles, tile), jnp.int32),
            pltpu.VMEM((n, 1, tile), jnp.int32),
            pltpu.VMEM((n, 1, tile), jnp.int32),
            pltpu.SMEM((n, 1, tile), jnp.int32),
            dma((3,)),
            dma((4,)),
            dma,
            dma,
            dma((n // RUN,)),
            dma((2,)),
            dma((2, len(CUTS) - 1)),
            dma((2, 2)),
            dma((2, 2)),
        ],
        compiler_params=pltpu.CompilerParams(
            collective_id=0, has_side_effects=True, vmem_limit_bytes=50 * 2**20
        ),
    )(
        *(
            pltpu.with_memory_space_constraint(x, pltpu.HBM)
            for x in (
                labels,
                band_w,
                far_w.reshape(n, slots * blk, tile),
                far_block[0].T,
                far_tile[0].T,
                far_count,
                seed_mask.reshape(tiles, tile),
            )
        )
    )
    return final, residual


def solution(mesh):
    placed = (
        P("node", None),
        P("node"),
        P("node", None, None, None),
        P("node", None, None),
        P("node", None, None),
        P("node", None),
        P("node", None, None, None, None),
    )
    return jax.shard_map(
        body,
        mesh=mesh,
        in_specs=placed,
        out_specs=(P("node", None), P(None, "node")),
        check_vma=False,
    )
```

```python
import functools

import jax
import jax.numpy as jnp
from jax import lax
from jax.experimental import pallas as pl
from jax.experimental.pallas import tpu as pltpu
from jax.sharding import PartitionSpec as P

MESH = pl.DeviceIdType.MESH
BF = jnp.bfloat16
F32 = jnp.float32
STEP = 91
BACK = 83
CHUNK = 16
FLOOR = 0.05
RUN = 8


def rows_of(start, size):
    return pl.ds(pl.multiple_of(start, size), size)


def fold_rows(change):
    rows, classes = change.shape
    total = jnp.sum(change.reshape(rows // 8, 8, classes), axis=0)
    return sum(total[:, i : i + 128] for i in range(0, classes, 128))


def close(tiles, tile, sub, new, old, first, out_hbm, res_hbm, second, res, copy_sem, res_sem):
    copy = pltpu.make_async_copy(new, out_hbm, copy_sem)
    copy.start()

    def change(t, carry):
        total = jnp.zeros((8, tile), F32)
        for j in range(tile // sub):
            low = t * tile + j * sub
            after = new[rows_of(low, sub), :].astype(F32)
            before = old[pl.ds(pl.multiple_of(tile + low, sub), sub), :].astype(F32)
            total = total + fold_rows(jnp.abs(after - before))
        second[t] = total
        return carry

    lax.fori_loop(0, tiles, change, 0)
    for it, part in enumerate((first, second)):
        block = jnp.concatenate([jnp.sum(part[...], axis=1), jnp.zeros((tile - tiles, tile), F32)], axis=0)
        res[it : it + 1, :] = jnp.sum(block.T, axis=0, keepdims=True)[:, :tiles]
    small = pltpu.make_async_copy(res, res_hbm, res_sem)
    small.start()
    small.wait()
    copy.wait()


def kernel(
    n, tiles, tile, classes, slots, blk,
    lab_hbm, bw_hbm, fw_hbm, fb_hbm, ft_hbm, fc_hbm, sm_hbm,
    out_ref, p1, resb,
    p0, g32, acc, halo, send, recv, bw, fw, wp, wt, mask, oh, dt, inv, sum0, sum1, sum2, sum3, fac0, fac1, fac2, fac3,
    fb, ft, fc, sm, req, qv, qs,
    load_sem, small_sem, req_ssem, req_rsem, q_sem, ssem, rsem, h_ssem, h_rsem,
):
    me = lax.axis_index("node")
    nodes = tiles * tile
    pair = slots * blk
    wide = n * pair
    sums, factors = (sum0, sum1, sum2, sum3), (fac0, fac1, fac2, fac3)
    chunks = n // CHUNK
    kdim = CHUNK * pair

    def plus(a, b):
        return (a + b) & (n - 1)

    def source_of(p):
        return plus(me, p * STEP)

    def target_of(p):
        return plus(me, -p * STEP)

    def far_first(i):
        return i ^ 84

    def each_peer(step):
        lax.fori_loop(0, 84, step, 0)
        lax.fori_loop(85, n, step, 0)

    small = [
        pltpu.make_async_copy(src, dst, small_sem.at[i])
        for i, (src, dst) in enumerate(((fb_hbm, fb), (ft_hbm, ft), (fc_hbm, fc), (sm_hbm, sm)))
    ]
    large = [
        pltpu.make_async_copy(fw_hbm, fw, load_sem.at[0]),
        pltpu.make_async_copy(lab_hbm, p0.at[pl.ds(tile, nodes)], load_sem.at[1]),
        pltpu.make_async_copy(bw_hbm, bw, load_sem.at[2]),
    ]
    for copy in small + large:
        copy.start()
    barrier = pltpu.get_barrier_semaphore()

    def greet(i, carry):
        pl.semaphore_signal(
            barrier, inc=1, device_id=(plus(me, far_first(i)),), device_id_type=MESH
        )
        return carry

    with jax.named_scope("s_greet"):
        each_peer(greet)
    for copy in small:
        copy.wait()

    lane = lax.broadcasted_iota(jnp.int32, (n, tile), 1)
    columns = [jnp.broadcast_to(fb[k : k + 1, :], (n, n)).T for k in range(slots)]
    table = jnp.where(lane == 0, columns[0], columns[1])
    for s in range(n):
        req[s] = table[s : s + 1]

    with jax.named_scope("s_barrier"):
        pl.semaphore_wait(barrier, n - 1)

    def ask(i, carry):
        distance = far_first(i)
        s = plus(me, distance)
        pltpu.make_async_remote_copy(
            req.at[s], qv.at[(distance * BACK) & (n - 1)], req_ssem, req_rsem,
            device_id=(s,), device_id_type=MESH,
        ).start()
        return carry

    with jax.named_scope("s_ask"):
        each_peer(ask)
    qv[0] = req[me]
    large[1].wait()

    nxt = plus(me, 1)
    prv = plus(me, n - 1)

    def halo_copies(it, cur, low=0, size=tile):
        part = pl.ds(low, size)
        up = pltpu.make_async_remote_copy(
            cur.at[pl.ds(nodes + low, size)], halo.at[it, 0, part], h_ssem.at[it, 0], h_rsem.at[it, 0],
            device_id=(nxt,), device_id_type=MESH,
        )
        down = pltpu.make_async_remote_copy(
            cur.at[pl.ds(tile + low, size)], halo.at[it, 1, part], h_ssem.at[it, 1], h_rsem.at[it, 1],
            device_id=(prv,), device_id_type=MESH,
        )
        return up, down

    halo0 = halo_copies(0, p0)
    for copy in halo0:
        copy.start()

    def widen(t, carry):
        rows = p0[rows_of(tile + t * tile, tile), :].astype(F32)
        g32[rows_of(t * (tile // blk), tile // blk)] = rows.reshape(tile // blk, blk, classes)
        return carry

    lax.fori_loop(0, tiles, widen, 0)
    edge = jnp.zeros((tile, classes), BF)
    for ref in (p0, p1):
        ref[pl.ds(0, tile), :] = edge
        ref[pl.ds(tile + nodes, tile), :] = edge

    large[0].wait()

    def place(p, carry):
        wp[p] = fw[source_of(p)]
        return carry

    lax.fori_loop(0, n, place, 0)

    def turn(j):
        part = wp[pl.ds(j * (tile // pair), tile // pair)].reshape(tile, tile)
        return part.astype(F32).T.astype(BF)

    def turn_chunk(c, carry):
        wt[c] = jnp.concatenate([turn(c * (kdim // tile) + j) for j in range(kdim // tile)], axis=1)
        return carry

    lax.fori_loop(0, chunks, turn_chunk, 0)

    row8 = lax.broadcasted_iota(jnp.int32, (8, n), 0)
    number = [jnp.where(fc[...] > k, ft[k : k + 1, :], -1) for k in range(slots)]
    numbers = jnp.where(row8 == 0, number[0], number[1]).astype(F32).astype(BF)
    step = 512

    def mark(j, carry):
        col = lax.broadcasted_iota(jnp.int32, (n, step), 1) + j * step
        src = (me + (col // pair) * STEP) & (n - 1)
        pick = jnp.where(lax.broadcasted_iota(jnp.int32, (n, step), 0) == src, 1.0, 0.0).astype(BF)
        found = jnp.dot(numbers, pick, preferred_element_type=F32)
        first = lax.rem(col[:1] // blk, slots) == 0
        mine = jnp.where(first, found[:1], found[1:2])
        ids = lax.broadcasted_iota(jnp.int32, (tiles, step), 0).astype(F32)
        oh[:, rows_of(j * step, step)] = jnp.where(mine == ids, 1.0, 0.0)
        return carry

    lax.fori_loop(0, wide // step, mark, 0)

    far_deg = jnp.dot(oh[...].astype(BF), wp[...].reshape(wide, tile), preferred_element_type=F32)
    seeds = sm[...].astype(F32)
    stack = jnp.concatenate([far_deg, seeds, jnp.zeros((tile - 2 * tiles, tile), F32)], axis=0)
    dt[...] = stack.T
    asked = pltpu.make_async_remote_copy(
        req.at[pl.ds(1, n - 1)], qv.at[pl.ds(1, n - 1)], req_ssem, req_rsem,
        device_id=(nxt,), device_id_type=MESH,
    )
    with jax.named_scope("s_waitreq"):
        asked.wait_recv()
    def to_scalar(g):
        span = pl.ds(g * RUN, RUN)
        return pltpu.make_async_copy(qv.at[span], qs.at[span], q_sem.at[g])

    runs = n // RUN
    for g in range(runs):
        to_scalar(g).start()

    def exchange(it):
        def gather(p):
            blocks = [g32[qs[p, 0, k]] for k in range(slots)]
            return jnp.concatenate(blocks, axis=0).astype(BF)

        def load(g, low=0):
            if it == 0:
                to_scalar(g).wait()
            for j in range(low, RUN):
                send[it, g * RUN + j] = gather(g * RUN + j)

        def ship(g, low=0):
            c = g // (CHUNK // RUN)
            for j in range(low, RUN):
                p = g * RUN + j
                pltpu.make_async_remote_copy(
                    send.at[it, p], recv.at[it, p], ssem.at[it], rsem.at[it, c],
                    device_id=(target_of(p),), device_id_type=MESH,
                ).start()

        def both(g, carry):
            load(g)
            ship(g - 1)
            if it == 1:
                low = pl.multiple_of((g // 2 - 1) * 16, 16)

                @pl.when(g % 2 == 0)
                def _():
                    for copy in halo_copies(1, p1, low, 16):
                        copy.start()

            return carry

        zero = jnp.int32(0)
        load(zero, 1)
        recv[it, 0] = gather(0)
        load(zero + 1)
        ship(zero, 1)
        lax.fori_loop(2, runs, both, 0)
        ship(zero + (runs - 1))
        if it == 1:
            for copy in halo_copies(1, p1, tile - 16, 16):
                copy.start()

    def band(cur, t):
        lhs = jnp.concatenate([bw[t, 0], bw[t, 1], bw[t, 2]], axis=1)
        rhs = cur[pl.ds(pl.multiple_of(t * tile, tile), 3 * tile), :]
        acc[rows_of(t * tile, tile), :] = jnp.dot(lhs, rhs, preferred_element_type=F32)

    def band_all(cur):
        def inner(i, carry):
            band(cur, 2 * i)
            band(cur, 2 * i + 1)
            return carry

        lax.fori_loop(0, tiles // 2, inner, 0)

    def edges(it, copies):
        for copy in copies:
            copy.wait_recv()
        for side, t, o in ((0, 0, 0), (1, tiles - 1, 2)):
            rows = pl.ds(t * tile, tile)
            acc[rows, :] = acc[rows, :] + jnp.dot(bw[t, o], halo[it, side], preferred_element_type=F32)

    def arrived(it, c, low=0):
        span = pl.ds(c * CHUNK + low, CHUNK - low)
        pltpu.make_async_remote_copy(
            send.at[it, span], recv.at[it, span], ssem.at[it], rsem.at[it, c],
            device_id=(nxt,), device_id_type=MESH,
        ).wait_recv()

    def product(it, c, t, count):
        rhs = recv[it, pl.ds(c * CHUNK, CHUNK)].reshape(kdim, classes)
        weights = wt[c].reshape(tile // 16, 16, kdim)
        parts = [(weights * mask[c, t + j][None]).reshape(tile, kdim) for j in range(count)]
        lhs = parts[0] if count == 1 else jnp.concatenate(parts, axis=0)
        return jnp.dot(lhs, rhs, preferred_element_type=F32)

    group = 16

    def far(it, copies):
        def chunk(c, carry):
            with jax.named_scope("s_wait"):
                arrived(it, c)
            multiply(c)
            return carry

        def multiply(c):
            def some(g, inner):
                rows = rows_of(g * group * tile, group * tile)
                acc[rows, :] = acc[rows, :] + product(it, c, g * group, group)
                return inner

            with jax.named_scope("s_mm"):
                lax.fori_loop(0, tiles // group, some, 0)

        arrived(it, 0, 1)
        multiply(jnp.int32(0))
        lax.fori_loop(1, chunks - 1, chunk, 0)
        edges(it, copies)
        with jax.named_scope("s_waitlast"):
            arrived(it, chunks - 1)

    sub = 32
    reps = classes // tile

    def scale(it, t, slot):
        spread = acc[rows_of(t * tile, tile), :] + product(it, chunks - 1, t, 1)
        sums[slot][...] = spread
        one = jnp.abs(inv[rows_of(t * tile, tile), :])
        square = jnp.sum(spread * spread, axis=1, keepdims=True)
        mean = square * one * one * (1.0 / classes)
        factors[slot][...] = one * lax.rsqrt(jnp.maximum(mean, FLOOR * FLOOR))

    def fresh(t, slot, j):
        part = pl.ds(j * sub, sub)
        row = t * tile + j * sub
        scaled = sums[slot][part, :] * jnp.concatenate([factors[slot][part, :]] * reps, axis=1)
        seeded = jnp.concatenate([inv[rows_of(row, sub), :]] * reps, axis=1) < 0.0
        given = p0[pl.ds(pl.multiple_of(tile + row, sub), sub), :].astype(F32)
        return jnp.where(seeded, given, scaled)

    fold = fold_rows

    def finish(it, write):
        def step(i, carry):
            t = 4 * i
            scale(it, t + 2, 2)
            scale(it, t + 3, 3)
            write(t, 0)
            write(t + 1, 1)
            scale(it, t + 4, 0)
            scale(it, t + 5, 1)
            write(t + 2, 2)
            write(t + 3, 3)
            return carry

        last = jnp.int32(tiles - 4)
        scale(it, jnp.int32(0), 0)
        scale(it, jnp.int32(1), 1)
        lax.fori_loop(0, tiles // 4 - 1, step, 0)
        scale(it, last + 2, 2)
        scale(it, last + 3, 3)
        for j in range(4):
            write(last + j, j)

    with jax.named_scope("s_exchange0"):
        exchange(0)

    large[2].wait()

    def invert(i, carry):
        both = dt[...]
        for k in range(4):
            t = i * 4 + k
            far = jnp.sum(jnp.where(lane == t, both, 0.0), axis=1, keepdims=True)
            seed = jnp.sum(jnp.where(lane == t + tiles, both, 0.0), axis=1, keepdims=True)
            weight = bw[t, 0].astype(F32) + bw[t, 1].astype(F32) + bw[t, 2].astype(F32)
            one = 1.0 / (jnp.sum(weight, axis=1, keepdims=True) + far)
            inv[rows_of(t * tile, tile), :] = jnp.broadcast_to(jnp.where(seed > 0.5, -one, one), (tile, tile))
        return carry

    with jax.named_scope("s_invert"):
        lax.fori_loop(0, tiles // 4, invert, 0)

    def spread_mask(c, carry):
        def some(i, inner):
            rows = oh[rows_of(i * 8, 8), rows_of(c * kdim, kdim)]
            for j in range(8):
                mask[c, i * 8 + j] = jnp.broadcast_to(rows[j : j + 1], (16, kdim)).astype(BF)
            return inner

        lax.fori_loop(0, tiles // 8, some, 0)
        return carry

    with jax.named_scope("s_mask"):
        lax.fori_loop(0, chunks, spread_mask, 0)
    with jax.named_scope("s_band0"):
        band_all(p0)
    far(0, halo0)

    def write0(t, slot):
        for j in range(tile // sub):
            new = fresh(t, slot, j)
            g32[pl.ds(t * (tile // blk) + j * (sub // blk), sub // blk)] = new.reshape(sub // blk, blk, classes)

    with jax.named_scope("s_finish0"):
        finish(0, write0)

    def narrow(t):
        new = g32[rows_of(t * (tile // blk), tile // blk)].reshape(tile, classes).astype(BF)
        p1[rows_of(tile + t * tile, tile), :] = new

    narrow(jnp.int32(0))
    narrow(jnp.int32(tiles - 1))

    halo1 = halo_copies(1, p1)
    with jax.named_scope("s_exchange1"):
        exchange(1)

    def change0(t, carry):
        total = jnp.zeros((8, tile), F32)
        for j in range(tile // sub):
            rows = pl.ds(pl.multiple_of(tile + t * tile + j * sub, sub), sub)
            part = pl.ds(t * (tile // blk) + j * (sub // blk), sub // blk)
            new = g32[part].reshape(sub, classes).astype(BF)
            p1[rows, :] = new
            total = total + fold(jnp.abs(new.astype(F32) - p0[rows, :].astype(F32)))
        resb[t] = total
        return carry

    def edge_change(t):
        total = jnp.zeros((8, tile), F32)
        for j in range(tile // sub):
            rows = pl.ds(tile + t * tile + j * sub, sub)
            total = total + fold(jnp.abs(p1[rows, :].astype(F32) - p0[rows, :].astype(F32)))
        resb[t] = total

    with jax.named_scope("s_change0"):
        lax.fori_loop(1, tiles - 1, change0, 0)
        edge_change(0)
        edge_change(tiles - 1)
    with jax.named_scope("s_band1"):
        band_all(p1)
    far(1, halo1)

    def write1(t, slot):
        for j in range(tile // sub):
            out_ref[rows_of(t * tile + j * sub, sub), :] = fresh(t, slot, j).astype(BF)

    with jax.named_scope("s_finish1"):
        finish(1, write1)

    asked.wait_send()
    for copy in halo0 + halo1:
        copy.wait_send()
    for it in range(2):
        span = pl.ds(1, n - 1)
        pltpu.make_async_remote_copy(
            send.at[it, span], recv.at[it, span], ssem.at[it], rsem.at[it, 0],
            device_id=(nxt,), device_id_type=MESH,
        ).wait_send()


def body(labels, seed_mask, band_w, far_block, far_tile, far_count, far_w):
    nodes, classes = labels.shape
    tiles, _, tile, _ = band_w.shape
    _, n, slots, blk, _ = far_w.shape
    hbm = pl.BlockSpec(memory_space=pltpu.HBM)
    vmem = pl.BlockSpec(memory_space=pltpu.VMEM)
    dma = pltpu.SemaphoreType.DMA
    wide = n * slots * blk
    new, old, first = pl.pallas_call(
        functools.partial(kernel, n, tiles, tile, classes, slots, blk),
        out_shape=(
            pltpu.VMEM((nodes, classes), BF),
            pltpu.VMEM((nodes + 2 * tile, classes), BF),
            pltpu.VMEM((tiles, 8, tile), F32),
        ),
        in_specs=[hbm] * 7,
        out_specs=(vmem, vmem, vmem),
        scratch_shapes=[
            pltpu.VMEM((nodes + 2 * tile, classes), BF),
            pltpu.VMEM((nodes // blk, blk, classes), F32),
            pltpu.VMEM((nodes, classes), F32),
            pltpu.VMEM((2, 2, tile, classes), BF),
            pltpu.VMEM((2, n, slots * blk, classes), BF),
            pltpu.VMEM((2, n, slots * blk, classes), BF),
            pltpu.VMEM(band_w.shape, BF),
            pltpu.VMEM((n, slots * blk, tile), BF),
            pltpu.VMEM((n, slots * blk, tile), BF),
            pltpu.VMEM((n // CHUNK, tile, CHUNK * slots * blk), BF),
            pltpu.VMEM((n // CHUNK, tiles, 16, CHUNK * slots * blk), BF),
            pltpu.VMEM((tiles, wide), F32),
            pltpu.VMEM((tile, tile), F32),
            pltpu.VMEM((nodes, tile), F32),
                *[pltpu.VMEM((tile, classes), F32)] * 4,
            *[pltpu.VMEM((tile, tile), F32)] * 4,
            pltpu.VMEM((slots, n), jnp.int32),
            pltpu.VMEM((slots, n), jnp.int32),
            pltpu.VMEM((1, n), jnp.int32),
            pltpu.VMEM((tiles, tile), jnp.int32),
            pltpu.VMEM((n, 1, tile), jnp.int32),
            pltpu.VMEM((n, 1, tile), jnp.int32),
            pltpu.SMEM((n, 1, tile), jnp.int32),
            dma((3,)),
            dma((4,)),
            dma,
            dma,
            dma((n // RUN,)),
            dma((2,)),
            dma((2, n // CHUNK)),
            dma((2, 2)),
            dma((2, 2)),
        ],
        compiler_params=pltpu.CompilerParams(
            collective_id=0, has_side_effects=True, vmem_limit_bytes=51 * 2**20
        ),
    )(
        *(
            pltpu.with_memory_space_constraint(x, pltpu.HBM)
            for x in (
                labels,
                band_w,
                far_w.reshape(n, slots * blk, tile),
                far_block[0].T,
                far_tile[0].T,
                far_count,
                seed_mask.reshape(tiles, tile),
            )
        )
    )
    return pl.pallas_call(
        functools.partial(close, tiles, tile, 32),
        out_shape=(
            jax.ShapeDtypeStruct((nodes, classes), BF),
            jax.ShapeDtypeStruct((2, tiles), F32),
        ),
        in_specs=[vmem] * 3,
        out_specs=(hbm, hbm),
        scratch_shapes=[
            pltpu.VMEM((tiles, 8, tile), F32),
            pltpu.VMEM((2, tiles), F32),
            dma,
            dma,
        ],
        compiler_params=pltpu.CompilerParams(vmem_limit_bytes=4 * 2**20),
    )(*(pltpu.with_memory_space_constraint(x, pltpu.VMEM) for x in (new, old, first)))


def solution(mesh):
    placed = (
        P("node", None),
        P("node"),
        P("node", None, None, None),
        P("node", None, None),
        P("node", None, None),
        P("node", None),
        P("node", None, None, None, None),
    )
    return jax.shard_map(
        body,
        mesh=mesh,
        in_specs=placed,
        out_specs=(P("node", None), P(None, "node")),
        check_vma=False,
    )
```

```python
import functools

import jax
import jax.numpy as jnp
from jax import lax
from jax.experimental import pallas as pl
from jax.experimental.pallas import tpu as pltpu
from jax.sharding import PartitionSpec as P

MESH = pl.DeviceIdType.MESH
BF = jnp.bfloat16
F32 = jnp.float32
STEP = 91
BACK = 83
CHUNK = 16
FLOOR = 0.05
RUN = 8


def rows_of(start, size):
    return pl.ds(pl.multiple_of(start, size), size)


def fold_rows(change):
    rows, classes = change.shape
    total = jnp.sum(change.reshape(rows // 8, 8, classes), axis=0)
    return sum(total[:, i : i + 128] for i in range(0, classes, 128))


def close(tiles, tile, sub, new, old, first, out_hbm, res_hbm, second, res, copy_sem, res_sem):
    copy = pltpu.make_async_copy(new, out_hbm, copy_sem)
    copy.start()

    def change(t, carry):
        total = jnp.zeros((8, tile), F32)
        for j in range(tile // sub):
            low = t * tile + j * sub
            after = new[rows_of(low, sub), :]
            before = old[pl.ds(pl.multiple_of(tile + low, sub), sub), :]
            total = total + fold_rows(jnp.abs(after - before).astype(F32))
        second[t] = total
        return carry

    lax.fori_loop(0, tiles, change, 0)
    for it, part in enumerate((first, second)):
        block = jnp.concatenate([jnp.sum(part[...], axis=1), jnp.zeros((tile - tiles, tile), F32)], axis=0)
        res[it : it + 1, :] = jnp.sum(block.T, axis=0, keepdims=True)[:, :tiles]
    small = pltpu.make_async_copy(res, res_hbm, res_sem)
    small.start()
    small.wait()
    copy.wait()


def kernel(
    n, tiles, tile, classes, slots, blk,
    lab_hbm, bw_hbm, fw_hbm, fb_hbm, ft_hbm, fc_hbm, sm_hbm,
    out_ref, p1, resb,
    p0, g32, acc, halo, send, recv, bw, fw, wp, wt, mask, oh, dt, inv, sum0, sum1, sum2, sum3, sum4, sum5, sum6, sum7,
    fac0, fac1, fac2, fac3, fac4, fac5, fac6, fac7,
    fb, ft, fc, sm, req, qv, qs,
    load_sem, small_sem, req_ssem, req_rsem, q_sem, ssem, rsem, h_ssem, h_rsem,
):
    me = lax.axis_index("node")
    nodes = tiles * tile
    pair = slots * blk
    wide = n * pair
    def get(ref, row, size):
        part = pl.ds(pl.multiple_of(row // blk, size // blk), size // blk)
        return ref[part].reshape(size, ref.shape[2])

    def put(ref, row, size, value):
        part = pl.ds(pl.multiple_of(row // blk, size // blk), size // blk)
        ref[part] = value.reshape(size // blk, blk, ref.shape[2])

    sums = (sum0, sum1, sum2, sum3, sum4, sum5, sum6, sum7)
    factors = (fac0, fac1, fac2, fac3, fac4, fac5, fac6, fac7)
    chunks = n // CHUNK
    kdim = CHUNK * pair

    def plus(a, b):
        return (a + b) & (n - 1)

    def source_of(p):
        return plus(me, p * STEP)

    def target_of(p):
        return plus(me, -p * STEP)

    def far_first():
        def hops(s):
            return sum(min(s // d % 4, 4 - s // d % 4) for d in (2, 8, 32))

        return sorted(range(1, n), key=lambda s: (-hops(s), s))

    small = [
        pltpu.make_async_copy(src, dst, small_sem.at[i])
        for i, (src, dst) in enumerate(((fb_hbm, fb), (ft_hbm, ft), (fc_hbm, fc), (sm_hbm, sm)))
    ]
    large = [
        pltpu.make_async_copy(fw_hbm, fw, load_sem.at[0]),
        pltpu.make_async_copy(lab_hbm, p0.at[pl.ds(tile, nodes)], load_sem.at[1]),
        pltpu.make_async_copy(bw_hbm, bw, load_sem.at[2]),
    ]
    for copy in small + large:
        copy.start()
    barrier = pltpu.get_barrier_semaphore()

    with jax.named_scope("s_greet"):
        for distance in far_first():
            pl.semaphore_signal(barrier, inc=1, device_id=(plus(me, distance),), device_id_type=MESH)
    for copy in small:
        copy.wait()

    lane = lax.broadcasted_iota(jnp.int32, (n, tile), 1)
    columns = [jnp.broadcast_to(fb[k : k + 1, :], (n, n)).T for k in range(slots)]
    table = jnp.where(lane == 0, columns[0], columns[1])
    for s in range(n):
        req[s] = table[s : s + 1]

    with jax.named_scope("s_barrier"):
        pl.semaphore_wait(barrier, n - 1)

    with jax.named_scope("s_ask"):
        for distance in far_first():
            s = plus(me, distance)
            pltpu.make_async_remote_copy(
                req.at[s], qv.at[distance * BACK % n], req_ssem, req_rsem, device_id=(s,), device_id_type=MESH
            ).start()
    qv[0] = req[me]
    large[1].wait()

    nxt = plus(me, 1)
    prv = plus(me, n - 1)

    def halo_copies(it, cur, low=0, size=tile):
        part = pl.ds(low, size)
        up = pltpu.make_async_remote_copy(
            cur.at[pl.ds(nodes + low, size)], halo.at[it, 0, part], h_ssem.at[it, 0], h_rsem.at[it, 0],
            device_id=(nxt,), device_id_type=MESH,
        )
        down = pltpu.make_async_remote_copy(
            cur.at[pl.ds(tile + low, size)], halo.at[it, 1, part], h_ssem.at[it, 1], h_rsem.at[it, 1],
            device_id=(prv,), device_id_type=MESH,
        )
        return up, down

    halo0 = halo_copies(0, p0)
    for copy in halo0:
        copy.start()

    def widen(t, carry):
        rows = p0[rows_of(tile + t * tile, tile), :].astype(F32)
        g32[rows_of(t * (tile // blk), tile // blk)] = rows.reshape(tile // blk, blk, classes)
        return carry

    lax.fori_loop(0, tiles, widen, 0)
    edge = jnp.zeros((tile, classes), BF)
    for ref in (p0, p1):
        ref[pl.ds(0, tile), :] = edge
        ref[pl.ds(tile + nodes, tile), :] = edge

    large[0].wait()

    def place(p, carry):
        wp[p] = fw[source_of(p)]
        return carry

    lax.fori_loop(0, n, place, 0)

    def turn(j):
        part = wp[pl.ds(j * (tile // pair), tile // pair)].reshape(tile, tile)
        return part.astype(F32).T.astype(BF)

    def turn_chunk(c, carry):
        wt[c] = jnp.concatenate([turn(c * (kdim // tile) + j) for j in range(kdim // tile)], axis=1)
        return carry

    lax.fori_loop(0, chunks, turn_chunk, 0)

    row8 = lax.broadcasted_iota(jnp.int32, (8, n), 0)
    number = [jnp.where(fc[...] > k, ft[k : k + 1, :], -1) for k in range(slots)]
    numbers = jnp.where(row8 == 0, number[0], number[1]).astype(F32).astype(BF)
    step = 512

    def mark(j, carry):
        col = lax.broadcasted_iota(jnp.int32, (n, step), 1) + j * step
        src = (me + (col // pair) * STEP) & (n - 1)
        pick = jnp.where(lax.broadcasted_iota(jnp.int32, (n, step), 0) == src, 1.0, 0.0).astype(BF)
        found = jnp.dot(numbers, pick, preferred_element_type=F32)
        first = lax.rem(col[:1] // blk, slots) == 0
        mine = jnp.where(first, found[:1], found[1:2])
        ids = lax.broadcasted_iota(jnp.int32, (tiles, step), 0).astype(F32)
        oh[:, rows_of(j * step, step)] = jnp.where(mine == ids, 1.0, 0.0)
        return carry

    lax.fori_loop(0, wide // step, mark, 0)

    far_deg = jnp.dot(oh[...].astype(BF), wp[...].reshape(wide, tile), preferred_element_type=F32)
    seeds = sm[...].astype(F32)
    stack = jnp.concatenate([far_deg, seeds, jnp.zeros((tile - 2 * tiles, tile), F32)], axis=0)
    dt[...] = stack.T
    asked = pltpu.make_async_remote_copy(
        req.at[pl.ds(1, n - 1)], qv.at[pl.ds(1, n - 1)], req_ssem, req_rsem,
        device_id=(nxt,), device_id_type=MESH,
    )
    with jax.named_scope("s_waitreq"):
        asked.wait_recv()
    def to_scalar(g):
        span = pl.ds(g * RUN, RUN)
        return pltpu.make_async_copy(qv.at[span], qs.at[span], q_sem.at[g])

    runs = n // RUN
    for g in range(runs):
        to_scalar(g).start()

    def band(cur, t):
        lhs = jnp.concatenate([bw[t, 0], bw[t, 1], bw[t, 2]], axis=1)
        rhs = cur[pl.ds(pl.multiple_of(t * tile, tile), 3 * tile), :]
        put(acc, t * tile, tile, jnp.dot(lhs, rhs, preferred_element_type=F32))

    def band_all(cur):
        def inner(i, carry):
            band(cur, 2 * i)
            band(cur, 2 * i + 1)
            return carry

        lax.fori_loop(0, tiles // 2, inner, 0)

    def edges(it, copies):
        for copy in copies:
            copy.wait_recv()
        for side, t, o in ((0, 0, 0), (1, tiles - 1, 2)):
            more = jnp.dot(bw[t, o], halo[it, side], preferred_element_type=F32)
            put(acc, t * tile, tile, get(acc, t * tile, tile) + more)

    def arrived(it, c, low=0):
        span = pl.ds(c * CHUNK + low, CHUNK - low)
        pltpu.make_async_remote_copy(
            send.at[it, span], recv.at[it, span], ssem.at[it], rsem.at[it, c],
            device_id=(nxt,), device_id_type=MESH,
        ).wait_recv()

    def product(it, c, t, count):
        rhs = recv[it, pl.ds(c * CHUNK, CHUNK)].reshape(kdim, classes)
        weights = wt[c].reshape(tile // 16, 16, kdim)
        parts = [(weights * mask[c, t + j][None]).reshape(tile, kdim) for j in range(count)]
        lhs = parts[0] if count == 1 else jnp.concatenate(parts, axis=0)
        return jnp.dot(lhs, rhs, preferred_element_type=F32)

    group = 16

    def multiply(it, c):
        def some(g, inner):
            row, size = g * group * tile, group * tile
            put(acc, row, size, get(acc, row, size) + product(it, c, g * group, group))
            return inner

        with jax.named_scope("s_mm"):
            lax.fori_loop(0, tiles // group, some, 0)

    def far(it, copies):
        def chunk(c, carry):
            with jax.named_scope("s_wait"):
                arrived(it, c)
            multiply(it, c)
            return carry

        arrived(it, 0, 1)
        multiply(it, jnp.int32(0))
        lax.fori_loop(1, chunks - 1, chunk, 0)
        edges(it, copies)
        with jax.named_scope("s_waitlast"):
            arrived(it, chunks - 1)

    sub = 32
    reps = classes // tile

    def factor_of(spread, one):
        square = jnp.sum(spread * spread, axis=1, keepdims=True)
        mean = square * one * one * (1.0 / classes)
        return one * lax.rsqrt(jnp.maximum(mean, FLOOR * FLOOR))

    def chosen(spread, factor, signed, given):
        seeded = jnp.concatenate([signed] * reps, axis=1) < 0.0
        return jnp.where(seeded, given, spread * jnp.concatenate([factor] * reps, axis=1))

    def scale(it, t, slot):
        spread = get(acc, t * tile, 2 * tile) + product(it, chunks - 1, t, 2)
        factor = factor_of(spread, jnp.abs(get(inv, t * tile, 2 * tile)))
        for k in range(2):
            part = slice(k * tile, (k + 1) * tile)
            sums[slot + k][...] = spread[part]
            factors[slot + k][...] = factor[part]

    def fresh(t, slot, j):
        part = pl.ds(j * sub, sub)
        row = t * tile + j * sub
        given = p0[pl.ds(pl.multiple_of(tile + row, sub), sub), :].astype(F32)
        return chosen(sums[slot][part, :], factors[slot][part, :], get(inv, row, sub), given)

    fold = fold_rows

    def settle(t):
        total = jnp.zeros((8, tile), F32)
        for j in range(tile // sub):
            row = t * tile + j * sub
            rows = pl.ds(pl.multiple_of(tile + row, sub), sub)
            spread, signed = get(acc, row, sub), get(inv, row, sub)
            given = p0[rows, :].astype(F32)
            new = chosen(spread, factor_of(spread, jnp.abs(signed)), signed, given).astype(BF)
            p1[rows, :] = new
            total = total + fold(jnp.abs(new.astype(F32) - given))
        resb[t] = total

    def exchange(it):
        def block(b):
            if it == 0:
                return g32[b]
            spread, signed = acc[b], inv[b]
            return chosen(spread, factor_of(spread, jnp.abs(signed)), signed, g32[b])

        def gather(p):
            return jnp.concatenate([block(qs[p, 0, k]) for k in range(slots)], axis=0).astype(BF)

        def load(g, low=0):
            if it == 0:
                to_scalar(g).wait()
            for j in range(low, RUN):
                send[it, g * RUN + j] = gather(g * RUN + j)

        def ship(g, low=0):
            c = g // (CHUNK // RUN)
            for j in range(low, RUN):
                p = g * RUN + j
                pltpu.make_async_remote_copy(
                    send.at[it, p], recv.at[it, p], ssem.at[it], rsem.at[it, c],
                    device_id=(target_of(p),), device_id_type=MESH,
                ).start()

        def both(g, carry):
            load(g)
            ship(g - 1)
            return carry

        def both_and_halo(g, carry):
            low = pl.multiple_of((g - runs // 2) * 16, 16)
            for copy in halo_copies(1, p1, low, 16):
                copy.start()
            return both(g, carry)

        zero = jnp.int32(0)
        load(zero, 1)
        recv[it, 0] = gather(0)
        load(zero + 1)
        ship(zero, 1)
        if it == 0:
            lax.fori_loop(2, runs, both, 0)
        else:
            lax.fori_loop(2, runs // 2, both, 0)
            with jax.named_scope("s_edgetiles"):
                settle(0)
                settle(tiles - 1)
            lax.fori_loop(runs // 2, runs, both_and_halo, 0)
        ship(zero + (runs - 1))

    def finish(it, write):
        def step(i, carry):
            t = 8 * i
            for j in (0, 2):
                scale(it, t + 4 + j, 4 + j)
                write(t + j, j)
                write(t + j + 1, j + 1)
            for j in (0, 2):
                scale(it, t + 8 + j, j)
                write(t + 4 + j, 4 + j)
                write(t + 5 + j, 5 + j)
            return carry

        for j in (0, 2):
            scale(it, jnp.int32(j), j)
        lax.fori_loop(0, tiles // 8 - 1, step, 0)
        t = jnp.int32(tiles - 8)
        for j in (0, 2):
            scale(it, t + 4 + j, 4 + j)
            write(t + j, j)
            write(t + j + 1, j + 1)
        for j in range(4):
            write(t + 4 + j, 4 + j)

    with jax.named_scope("s_exchange0"):
        exchange(0)

    large[2].wait()

    def invert(i, carry):
        both = dt[...]
        for k in range(4):
            t = i * 4 + k
            far = jnp.sum(jnp.where(lane == t, both, 0.0), axis=1, keepdims=True)
            seed = jnp.sum(jnp.where(lane == t + tiles, both, 0.0), axis=1, keepdims=True)
            weight = bw[t, 0].astype(F32) + bw[t, 1].astype(F32) + bw[t, 2].astype(F32)
            one = 1.0 / (jnp.sum(weight, axis=1, keepdims=True) + far)
            put(inv, t * tile, tile, jnp.broadcast_to(jnp.where(seed > 0.5, -one, one), (tile, tile)))
        return carry

    with jax.named_scope("s_invert"):
        lax.fori_loop(0, tiles // 4, invert, 0)

    def spread_mask(c, carry):
        def some(i, inner):
            rows = oh[rows_of(i * 8, 8), rows_of(c * kdim, kdim)]
            for j in range(8):
                mask[c, i * 8 + j] = jnp.broadcast_to(rows[j : j + 1], (16, kdim)).astype(BF)
            return inner

        lax.fori_loop(0, tiles // 8, some, 0)
        return carry

    with jax.named_scope("s_mask"):
        lax.fori_loop(0, chunks, spread_mask, 0)
    with jax.named_scope("s_band0"):
        band_all(p0)
    far(0, halo0)

    multiply(0, jnp.int32(chunks - 1))

    halo1 = halo_copies(1, p1)
    with jax.named_scope("s_exchange1"):
        exchange(1)

    def settle_two(i, carry):
        settle(2 * i + 1)
        settle(2 * i + 2)
        return carry

    with jax.named_scope("s_settle"):
        lax.fori_loop(0, tiles // 2 - 1, settle_two, 0)
    with jax.named_scope("s_band1"):
        band_all(p1)
    far(1, halo1)

    def write1(t, slot):
        for j in range(tile // sub):
            out_ref[rows_of(t * tile + j * sub, sub), :] = fresh(t, slot, j).astype(BF)

    with jax.named_scope("s_finish1"):
        finish(1, write1)

    asked.wait_send()
    for copy in halo0 + halo1:
        copy.wait_send()
    for it in range(2):
        span = pl.ds(1, n - 1)
        pltpu.make_async_remote_copy(
            send.at[it, span], recv.at[it, span], ssem.at[it], rsem.at[it, 0],
            device_id=(nxt,), device_id_type=MESH,
        ).wait_send()


def body(labels, seed_mask, band_w, far_block, far_tile, far_count, far_w):
    nodes, classes = labels.shape
    tiles, _, tile, _ = band_w.shape
    _, n, slots, blk, _ = far_w.shape
    hbm = pl.BlockSpec(memory_space=pltpu.HBM)
    vmem = pl.BlockSpec(memory_space=pltpu.VMEM)
    dma = pltpu.SemaphoreType.DMA
    wide = n * slots * blk
    new, old, first = pl.pallas_call(
        functools.partial(kernel, n, tiles, tile, classes, slots, blk),
        out_shape=(
            pltpu.VMEM((nodes, classes), BF),
            pltpu.VMEM((nodes + 2 * tile, classes), BF),
            pltpu.VMEM((tiles, 8, tile), F32),
        ),
        in_specs=[hbm] * 7,
        out_specs=(vmem, vmem, vmem),
        scratch_shapes=[
            pltpu.VMEM((nodes + 2 * tile, classes), BF),
            pltpu.VMEM((nodes // blk, blk, classes), F32),
            pltpu.VMEM((nodes // blk, blk, classes), F32),
            pltpu.VMEM((2, 2, tile, classes), BF),
            pltpu.VMEM((2, n, slots * blk, classes), BF),
            pltpu.VMEM((2, n, slots * blk, classes), BF),
            pltpu.VMEM(band_w.shape, BF),
            pltpu.VMEM((n, slots * blk, tile), BF),
            pltpu.VMEM((n, slots * blk, tile), BF),
            pltpu.VMEM((n // CHUNK, tile, CHUNK * slots * blk), BF),
            pltpu.VMEM((n // CHUNK, tiles, 16, CHUNK * slots * blk), BF),
            pltpu.VMEM((tiles, wide), F32),
            pltpu.VMEM((tile, tile), F32),
            pltpu.VMEM((nodes // blk, blk, tile), F32),
                *[pltpu.VMEM((tile, classes), F32)] * 8,
            *[pltpu.VMEM((tile, tile), F32)] * 8,
            pltpu.VMEM((slots, n), jnp.int32),
            pltpu.VMEM((slots, n), jnp.int32),
            pltpu.VMEM((1, n), jnp.int32),
            pltpu.VMEM((tiles, tile), jnp.int32),
            pltpu.VMEM((n, 1, tile), jnp.int32),
            pltpu.VMEM((n, 1, tile), jnp.int32),
            pltpu.SMEM((n, 1, tile), jnp.int32),
            dma((3,)),
            dma((4,)),
            dma,
            dma,
            dma((n // RUN,)),
            dma((2,)),
            dma((2, n // CHUNK)),
            dma((2, 2)),
            dma((2, 2)),
        ],
        compiler_params=pltpu.CompilerParams(
            collective_id=0, has_side_effects=True, vmem_limit_bytes=52 * 2**20
        ),
    )(
        *(
            pltpu.with_memory_space_constraint(x, pltpu.HBM)
            for x in (
                labels,
                band_w,
                far_w.reshape(n, slots * blk, tile),
                far_block[0].T,
                far_tile[0].T,
                far_count,
                seed_mask.reshape(tiles, tile),
            )
        )
    )
    return pl.pallas_call(
        functools.partial(close, tiles, tile, 32),
        out_shape=(
            jax.ShapeDtypeStruct((nodes, classes), BF),
            jax.ShapeDtypeStruct((2, tiles), F32),
        ),
        in_specs=[vmem] * 3,
        out_specs=(hbm, hbm),
        scratch_shapes=[
            pltpu.VMEM((tiles, 8, tile), F32),
            pltpu.VMEM((2, tiles), F32),
            dma,
            dma,
        ],
        compiler_params=pltpu.CompilerParams(vmem_limit_bytes=4 * 2**20),
    )(*(pltpu.with_memory_space_constraint(x, pltpu.VMEM) for x in (new, old, first)))


def solution(mesh):
    placed = (
        P("node", None),
        P("node"),
        P("node", None, None, None),
        P("node", None, None),
        P("node", None, None),
        P("node", None),
        P("node", None, None, None, None),
    )
    return jax.shard_map(
        body,
        mesh=mesh,
        in_specs=placed,
        out_specs=(P("node", None), P(None, "node")),
        check_vma=False,
    )
```

```python
import functools

import jax
import jax.numpy as jnp
from jax import lax
from jax.experimental import pallas as pl
from jax.experimental.pallas import tpu as pltpu
from jax.sharding import PartitionSpec as P

MESH = pl.DeviceIdType.MESH
BF = jnp.bfloat16
F32 = jnp.float32
STEP = 91
BACK = 83
CHUNK = 16
FLOOR = 0.05
RUN = 8


def rows_of(start, size):
    return pl.ds(pl.multiple_of(start, size), size)


def fold_rows(change):
    rows, classes = change.shape
    total = jnp.sum(change.reshape(rows // 8, 8, classes), axis=0)
    return sum(total[:, i : i + 128] for i in range(0, classes, 128))


def close(tiles, tile, sub, new, old, first, out_hbm, res_hbm, second, res, copy_sem, res_sem):
    copy = pltpu.make_async_copy(new, out_hbm, copy_sem)
    copy.start()

    def change(t, carry):
        total = jnp.zeros((8, tile), F32)
        for j in range(tile // sub):
            low = t * tile + j * sub
            after = new[rows_of(low, sub), :]
            before = old[pl.ds(pl.multiple_of(tile + low, sub), sub), :]
            total = total + fold_rows(jnp.abs(after - before).astype(F32))
        second[t] = total
        return carry

    lax.fori_loop(0, tiles, change, 0)
    for it, part in enumerate((first, second)):
        block = jnp.concatenate([jnp.sum(part[...], axis=1), jnp.zeros((tile - tiles, tile), F32)], axis=0)
        res[it : it + 1, :] = jnp.sum(block.T, axis=0, keepdims=True)[:, :tiles]
    small = pltpu.make_async_copy(res, res_hbm, res_sem)
    small.start()
    small.wait()
    copy.wait()


def kernel(
    n, tiles, tile, classes, slots, blk,
    lab_hbm, bw_hbm, fw_hbm, fb_hbm, ft_hbm, fc_hbm, sm_hbm,
    out_ref, p1, resb,
    p0, g32, acc, halo, send, recv, fsend, frecv, wf, bw, fw, wp, wt, mask, oh, dt, inv, sum0, sum1, sum2, sum3, sum4, sum5, sum6, sum7,
    fac0, fac1, fac2, fac3, fac4, fac5, fac6, fac7,
    fb, ft, fc, sm, req, qv, qs,
    load_sem, small_sem, req_ssem, req_rsem, q_sem, ssem, rsem, f_ssem, f_rsem, h_ssem, h_rsem,
):
    me = lax.axis_index("node")
    nodes = tiles * tile
    pair = slots * blk
    wide = n * pair
    def get(ref, row, size):
        part = pl.ds(pl.multiple_of(row // blk, size // blk), size // blk)
        return ref[part].reshape(size, ref.shape[2])

    def put(ref, row, size, value):
        part = pl.ds(pl.multiple_of(row // blk, size // blk), size // blk)
        ref[part] = value.reshape(size // blk, blk, ref.shape[2])

    sums = (sum0, sum1, sum2, sum3, sum4, sum5, sum6, sum7)
    factors = (fac0, fac1, fac2, fac3, fac4, fac5, fac6, fac7)
    chunks = n // CHUNK
    half = classes // 2
    kdim = CHUNK * pair

    def plus(a, b):
        return (a + b) & (n - 1)

    def source_of(p):
        return plus(me, p * STEP)

    def target_of(p):
        return plus(me, -p * STEP)

    def far_first():
        def hops(s):
            return sum(min(s // d % 4, 4 - s // d % 4) for d in (2, 8, 32))

        return sorted(range(1, n), key=lambda s: (-hops(s), s))

    small = [
        pltpu.make_async_copy(src, dst, small_sem.at[i])
        for i, (src, dst) in enumerate(((fb_hbm, fb), (ft_hbm, ft), (fc_hbm, fc), (sm_hbm, sm)))
    ]
    large = [
        pltpu.make_async_copy(fw_hbm, fw, load_sem.at[0]),
        pltpu.make_async_copy(lab_hbm, p0.at[pl.ds(tile, nodes)], load_sem.at[1]),
        pltpu.make_async_copy(bw_hbm, bw, load_sem.at[2]),
    ]
    for copy in small + large:
        copy.start()
    barrier = pltpu.get_barrier_semaphore()

    with jax.named_scope("s_greet"):
        for distance in far_first():
            pl.semaphore_signal(barrier, inc=1, device_id=(plus(me, distance),), device_id_type=MESH)
    for copy in small:
        copy.wait()

    lane = lax.broadcasted_iota(jnp.int32, (n, tile), 1)
    columns = [jnp.broadcast_to(fb[k : k + 1, :], (n, n)).T for k in range(slots)]
    table = jnp.where(lane == 0, columns[0], columns[1])
    for s in range(n):
        req[s] = table[s : s + 1]

    with jax.named_scope("s_barrier"):
        pl.semaphore_wait(barrier, n - 1)

    with jax.named_scope("s_ask"):
        for distance in far_first():
            s = plus(me, distance)
            pltpu.make_async_remote_copy(
                req.at[s], qv.at[distance * BACK % n], req_ssem, req_rsem, device_id=(s,), device_id_type=MESH
            ).start()
    qv[0] = req[me]
    large[1].wait()

    nxt = plus(me, 1)
    prv = plus(me, n - 1)

    def halo_copies(it, cur, low=0, size=tile):
        part = pl.ds(low, size)
        up = pltpu.make_async_remote_copy(
            cur.at[pl.ds(nodes + low, size)], halo.at[it, 0, part], h_ssem.at[it, 0], h_rsem.at[it, 0],
            device_id=(nxt,), device_id_type=MESH,
        )
        down = pltpu.make_async_remote_copy(
            cur.at[pl.ds(tile + low, size)], halo.at[it, 1, part], h_ssem.at[it, 1], h_rsem.at[it, 1],
            device_id=(prv,), device_id_type=MESH,
        )
        return up, down

    halo0 = halo_copies(0, p0)
    for copy in halo0:
        copy.start()

    def widen(t, carry):
        rows = p0[rows_of(tile + t * tile, tile), :].astype(F32)
        g32[rows_of(t * (tile // blk), tile // blk)] = rows.reshape(tile // blk, blk, classes)
        return carry

    lax.fori_loop(0, tiles, widen, 0)
    edge = jnp.zeros((tile, classes), BF)
    for ref in (p0, p1):
        ref[pl.ds(0, tile), :] = edge
        ref[pl.ds(tile + nodes, tile), :] = edge

    large[0].wait()

    def place(p, carry):
        wp[p] = fw[source_of(p)]
        return carry

    lax.fori_loop(0, n, place, 0)

    def turn(j):
        part = wp[pl.ds(j * (tile // pair), tile // pair)].reshape(tile, tile)
        return part.astype(F32).T.astype(BF)

    def turn_chunk(c, carry):
        wt[c] = jnp.concatenate([turn(c * (kdim // tile) + j) for j in range(kdim // tile)], axis=1)
        return carry

    lax.fori_loop(0, chunks, turn_chunk, 0)

    row8 = lax.broadcasted_iota(jnp.int32, (8, n), 0)
    number = [jnp.where(fc[...] > k, ft[k : k + 1, :], -1) for k in range(slots)]
    numbers = jnp.where(row8 == 0, number[0], number[1]).astype(F32).astype(BF)
    step = 512

    def mark(j, carry):
        col = lax.broadcasted_iota(jnp.int32, (n, step), 1) + j * step
        src = (me + (col // pair) * STEP) & (n - 1)
        pick = jnp.where(lax.broadcasted_iota(jnp.int32, (n, step), 0) == src, 1.0, 0.0).astype(BF)
        found = jnp.dot(numbers, pick, preferred_element_type=F32)
        first = lax.rem(col[:1] // blk, slots) == 0
        mine = jnp.where(first, found[:1], found[1:2])
        ids = lax.broadcasted_iota(jnp.int32, (tiles, step), 0).astype(F32)
        oh[:, rows_of(j * step, step)] = jnp.where(mine == ids, 1.0, 0.0)
        return carry

    lax.fori_loop(0, wide // step, mark, 0)

    far_deg = jnp.dot(oh[...].astype(BF), wp[...].reshape(wide, tile), preferred_element_type=F32)
    seeds = sm[...].astype(F32)
    stack = jnp.concatenate([far_deg, seeds, jnp.zeros((tile - 2 * tiles, tile), F32)], axis=0)
    dt[...] = stack.T
    asked = pltpu.make_async_remote_copy(
        req.at[pl.ds(1, n - 1)], qv.at[pl.ds(1, n - 1)], req_ssem, req_rsem,
        device_id=(nxt,), device_id_type=MESH,
    )
    with jax.named_scope("s_waitreq"):
        asked.wait_recv()
    def to_scalar(g):
        span = pl.ds(g * RUN, RUN)
        return pltpu.make_async_copy(qv.at[span], qs.at[span], q_sem.at[g])

    runs = n // RUN
    for g in range(runs):
        to_scalar(g).start()

    def band(cur, t):
        lhs = jnp.concatenate([bw[t, 0], bw[t, 1], bw[t, 2]], axis=1)
        rhs = cur[pl.ds(pl.multiple_of(t * tile, tile), 3 * tile), :]
        put(acc, t * tile, tile, jnp.dot(lhs, rhs, preferred_element_type=F32))

    def band_all(cur):
        def inner(i, carry):
            band(cur, 2 * i)
            band(cur, 2 * i + 1)
            return carry

        lax.fori_loop(0, tiles // 2, inner, 0)

    def edges(it, copies):
        for copy in copies:
            copy.wait_recv()
        for side, t, o in ((0, 0, 0), (1, tiles - 1, 2)):
            more = jnp.dot(bw[t, o], halo[it, side], preferred_element_type=F32)
            put(acc, t * tile, tile, get(acc, t * tile, tile) + more)

    def arrived(it, h, c, low=0):
        span = pl.ds(c * CHUNK + low, CHUNK - low)
        pltpu.make_async_remote_copy(
            send.at[it, h, span], recv.at[it, h, span], ssem.at[it, h], rsem.at[it, h, c],
            device_id=(nxt,), device_id_type=MESH,
        ).wait_recv()

    def product(it, h, c, t, count):
        span = pl.ds(c * CHUNK, CHUNK)
        if h is None:
            rhs = jnp.concatenate([recv[it, k, span].reshape(kdim, half) for k in range(2)], axis=1)
        else:
            rhs = recv[it, h, span].reshape(kdim, half)
        weights = (wt if it == 0 else wf)[c].reshape(tile // 16, 16, kdim)
        parts = [(weights * mask[c, t + j][None]).reshape(tile, kdim) for j in range(count)]
        lhs = parts[0] if count == 1 else jnp.concatenate(parts, axis=0)
        return jnp.dot(lhs, rhs, preferred_element_type=F32)

    group = 16

    def multiply(it, h, c):
        cols = pl.ds(0, classes) if h is None else pl.ds(h * half, half)

        def some(g, inner):
            size = group * tile // blk
            part = pl.ds(pl.multiple_of(g * size, size), size)
            more = product(it, h, c, g * group, group)
            acc[part, :, cols] = acc[part, :, cols] + more.reshape(size, blk, more.shape[1])
            return inner

        with jax.named_scope("s_mm"):
            lax.fori_loop(0, tiles // group, some, 0)

    def far(it, h, count):
        halves = (0, 1) if h is None else (h,)

        def chunk(c, carry):
            with jax.named_scope("s_wait"):
                for k in halves:
                    arrived(it, k, c)
            multiply(it, h, c)
            return carry

        for k in halves:
            arrived(it, k, 0, 1)
        multiply(it, h, jnp.int32(0))
        lax.fori_loop(1, count, chunk, 0)

    sub = 32
    reps = classes // tile

    def lift(spread, one):
        square = jnp.sum(spread * spread, axis=1, keepdims=True)
        mean = square * one * one * (1.0 / classes)
        return lax.rsqrt(jnp.maximum(mean, FLOOR * FLOOR))

    def factor_of(spread, one):
        return one * lift(spread, one)

    def chosen(spread, factor, signed, given):
        reps = spread.shape[1] // tile
        seeded = jnp.concatenate([signed] * reps, axis=1) < 0.0
        return jnp.where(seeded, given, spread * jnp.concatenate([factor] * reps, axis=1))

    def scale(it, t, slot):
        spread = get(acc, t * tile, 2 * tile) + product(it, None, chunks - 1, t, 2)
        factor = factor_of(spread, jnp.abs(get(inv, t * tile, 2 * tile)))
        for k in range(2):
            part = slice(k * tile, (k + 1) * tile)
            sums[slot + k][...] = spread[part]
            factors[slot + k][...] = factor[part]

    def fresh(t, slot, j):
        part = pl.ds(j * sub, sub)
        row = t * tile + j * sub
        given = p0[pl.ds(pl.multiple_of(tile + row, sub), sub), :].astype(F32)
        return chosen(sums[slot][part, :], factors[slot][part, :], get(inv, row, sub), given)

    fold = fold_rows

    def settle(t):
        total = jnp.zeros((8, tile), F32)
        for j in range(tile // sub):
            row = t * tile + j * sub
            rows = pl.ds(pl.multiple_of(tile + row, sub), sub)
            spread, signed = get(acc, row, sub), get(inv, row, sub)
            given = p0[rows, :].astype(F32)
            new = chosen(spread, factor_of(spread, jnp.abs(signed)), signed, given).astype(BF)
            p1[rows, :] = new
            total = total + fold(jnp.abs(new.astype(F32) - given))
        resb[t] = total

    def ship(it, h, g, low=0):
        for j in range(low, RUN):
            p = g * RUN + j
            pltpu.make_async_remote_copy(
                send.at[it, h, p], recv.at[it, h, p], ssem.at[it, h], rsem.at[it, h, g // (CHUNK // RUN)],
                device_id=(target_of(p),), device_id_type=MESH,
            ).start()

    def pair_of(block, p):
        return jnp.concatenate([block(qs[p, 0, k]) for k in range(slots)], axis=0).astype(BF)

    zero = jnp.int32(0)

    def exchange_labels():
        def load(g, low=0):
            to_scalar(g).wait()
            for j in range(low, RUN):
                rows = pair_of(lambda b: g32[b], g * RUN + j)
                send[0, 0, g * RUN + j] = rows[:, :half]
                send[0, 1, g * RUN + j] = rows[:, half:]

        def both(g, carry):
            load(g)
            ship(0, 0, g - 1)
            return carry

        def rest(g, carry):
            ship(0, 1, g)
            return carry

        load(zero, 1)
        own = pair_of(lambda b: g32[b], 0)
        recv[0, 0, 0] = own[:, :half]
        recv[0, 1, 0] = own[:, half:]
        load(zero + 1)
        ship(0, 0, zero, 1)
        lax.fori_loop(2, runs, both, 0)
        ship(0, 0, zero + (runs - 1))
        ship(0, 1, zero, 1)
        lax.fori_loop(1, runs, rest, 0)

    def gather_averages(h, g, low=0):
        def block(b):
            signed = inv[b]
            cols = slice(h * half, (h + 1) * half)
            return chosen(acc[b][:, cols], jnp.abs(signed), signed, g32[b][:, cols])

        for j in range(low, RUN):
            send[1, h, g * RUN + j] = pair_of(block, g * RUN + j)
        if isinstance(g, int) and g == 0:
            recv[1, h, 0] = pair_of(block, 0)

    def exchange_averages(h):
        def both(g, carry):
            gather_averages(h, g)
            ship(1, h, g - 1)
            return carry

        def both_and_halo(g, carry):
            low = pl.multiple_of((g - runs // 2) * 16, 16)
            for copy in halo_copies(1, p1, low, 16):
                copy.start()
            return both(g, carry)

        gather_averages(h, 0, 1)
        gather_averages(h, zero + 1)
        ship(1, h, zero, 1)
        lax.fori_loop(2, runs // 2, both, 0)
        if h == 1:
            settle(0)
            settle(tiles - 1)
        lax.fori_loop(runs // 2, runs, both_and_halo if h == 1 else both, 0)
        ship(1, h, zero + (runs - 1))

    def exchange_lifts():
        def load(g, carry):
            lifts = []
            for j in range(RUN):
                for k in range(slots):
                    b = qs[g * RUN + j, 0, k]
                    signed = inv[b]
                    lifts.append(jnp.where(signed < 0.0, 1.0, lift(acc[b], jnp.abs(signed))))
            fsend[g] = jnp.concatenate(lifts, axis=0).T[:1]
            return carry

        def tell(g, low=0):
            for j in range(low, RUN):
                p = g * RUN + j
                pltpu.make_async_remote_copy(
                    fsend.at[g], frecv.at[p], f_ssem, f_rsem, device_id=(target_of(p),), device_id_type=MESH
                ).start()

        def load_and_tell(g, carry):
            load(g, carry)
            tell(g - 1)
            return carry

        load(zero, 0)
        frecv[0] = fsend[0]
        load(zero + 1, 0)
        tell(zero, 1)
        lax.fori_loop(2, runs, load_and_tell, 0)
        tell(zero + (runs - 1))

    def told():
        pltpu.make_async_remote_copy(
            frecv.at[pl.ds(1, n - 1)], frecv.at[pl.ds(1, n - 1)], f_ssem, f_rsem,
            device_id=(nxt,), device_id_type=MESH,
        ).wait_recv()
        place_of = lax.broadcasted_iota(jnp.int32, (1, tile), 1) // pair

        def apply(c, carry):
            lanes = []
            for i in range(CHUNK // RUN):
                row = jnp.zeros((1, tile), F32)
                for j in range(RUN):
                    row = jnp.where(place_of == j, frecv[c * CHUNK + i * RUN + j], row)
                lanes.append(row)
            wf[c] = (wt[c].astype(F32) * jnp.concatenate(lanes, axis=1)).astype(BF)
            return carry

        lax.fori_loop(0, chunks, apply, 0)

    def finish(it, write):
        def step(i, carry):
            t = 8 * i
            for j in (0, 2):
                scale(it, t + 4 + j, 4 + j)
                write(t + j, j)
                write(t + j + 1, j + 1)
            for j in (0, 2):
                scale(it, t + 8 + j, j)
                write(t + 4 + j, 4 + j)
                write(t + 5 + j, 5 + j)
            return carry

        for j in (0, 2):
            scale(it, jnp.int32(j), j)
        lax.fori_loop(0, tiles // 8 - 1, step, 0)
        t = jnp.int32(tiles - 8)
        for j in (0, 2):
            scale(it, t + 4 + j, 4 + j)
            write(t + j, j)
            write(t + j + 1, j + 1)
        for j in range(4):
            write(t + 4 + j, 4 + j)

    with jax.named_scope("s_exchange0"):
        exchange_labels()

    large[2].wait()

    def invert(i, carry):
        both = dt[...]
        for k in range(4):
            t = i * 4 + k
            far = jnp.sum(jnp.where(lane == t, both, 0.0), axis=1, keepdims=True)
            seed = jnp.sum(jnp.where(lane == t + tiles, both, 0.0), axis=1, keepdims=True)
            weight = bw[t, 0].astype(F32) + bw[t, 1].astype(F32) + bw[t, 2].astype(F32)
            one = 1.0 / (jnp.sum(weight, axis=1, keepdims=True) + far)
            put(inv, t * tile, tile, jnp.broadcast_to(jnp.where(seed > 0.5, -one, one), (tile, tile)))
        return carry

    with jax.named_scope("s_invert"):
        lax.fori_loop(0, tiles // 4, invert, 0)

    def spread_mask(c, carry):
        def some(i, inner):
            rows = oh[rows_of(i * 8, 8), rows_of(c * kdim, kdim)]
            for j in range(8):
                mask[c, i * 8 + j] = jnp.broadcast_to(rows[j : j + 1], (16, kdim)).astype(BF)
            return inner

        lax.fori_loop(0, tiles // 8, some, 0)
        return carry

    with jax.named_scope("s_mask"):
        lax.fori_loop(0, chunks, spread_mask, 0)
    with jax.named_scope("s_band0"):
        band_all(p0)
    far(0, 0, chunks)
    edges(0, halo0)
    with jax.named_scope("s_averages"):
        exchange_averages(0)
    far(0, 1, chunks)

    halo1 = halo_copies(1, p1)
    with jax.named_scope("s_exchange1"):
        exchange_lifts()
        with jax.named_scope("s_second"):
            exchange_averages(1)

    def settle_five(i, carry):
        for j in range(5):
            settle(5 * i + 1 + j)
        return carry

    with jax.named_scope("s_settle"):
        lax.fori_loop(0, (tiles - 2) // 5, settle_five, 0)
    with jax.named_scope("s_band1"):
        band_all(p1)
    with jax.named_scope("s_told"):
        told()
    far(1, None, chunks - 1)
    edges(1, halo1)
    with jax.named_scope("s_waitlast"):
        for h in range(2):
            arrived(1, h, chunks - 1)

    def write1(t, slot):
        for j in range(tile // sub):
            out_ref[rows_of(t * tile + j * sub, sub), :] = fresh(t, slot, j).astype(BF)

    with jax.named_scope("s_finish1"):
        finish(1, write1)

    asked.wait_send()
    for copy in halo0 + halo1:
        copy.wait_send()
    span = pl.ds(1, n - 1)
    for it in range(2):
        for h in range(2):
            pltpu.make_async_remote_copy(
                send.at[it, h, span], recv.at[it, h, span], ssem.at[it, h], rsem.at[it, h, 0],
                device_id=(nxt,), device_id_type=MESH,
            ).wait_send()
    pltpu.make_async_remote_copy(
        frecv.at[span], frecv.at[span], f_ssem, f_rsem, device_id=(nxt,), device_id_type=MESH
    ).wait_send()


def body(labels, seed_mask, band_w, far_block, far_tile, far_count, far_w):
    nodes, classes = labels.shape
    tiles, _, tile, _ = band_w.shape
    _, n, slots, blk, _ = far_w.shape
    hbm = pl.BlockSpec(memory_space=pltpu.HBM)
    vmem = pl.BlockSpec(memory_space=pltpu.VMEM)
    dma = pltpu.SemaphoreType.DMA
    wide = n * slots * blk
    new, old, first = pl.pallas_call(
        functools.partial(kernel, n, tiles, tile, classes, slots, blk),
        out_shape=(
            pltpu.VMEM((nodes, classes), BF),
            pltpu.VMEM((nodes + 2 * tile, classes), BF),
            pltpu.VMEM((tiles, 8, tile), F32),
        ),
        in_specs=[hbm] * 7,
        out_specs=(vmem, vmem, vmem),
        scratch_shapes=[
            pltpu.VMEM((nodes + 2 * tile, classes), BF),
            pltpu.VMEM((nodes // blk, blk, classes), F32),
            pltpu.VMEM((nodes // blk, blk, classes), F32),
            pltpu.VMEM((2, 2, tile, classes), BF),
            pltpu.VMEM((2, 2, n, slots * blk, classes // 2), BF),
            pltpu.VMEM((2, 2, n, slots * blk, classes // 2), BF),
            pltpu.VMEM((n // RUN, 1, tile), F32),
            pltpu.VMEM((n, 1, tile), F32),
            pltpu.VMEM((n // CHUNK, tile, CHUNK * slots * blk), BF),
            pltpu.VMEM(band_w.shape, BF),
            pltpu.VMEM((n, slots * blk, tile), BF),
            pltpu.VMEM((n, slots * blk, tile), BF),
            pltpu.VMEM((n // CHUNK, tile, CHUNK * slots * blk), BF),
            pltpu.VMEM((n // CHUNK, tiles, 16, CHUNK * slots * blk), BF),
            pltpu.VMEM((tiles, wide), F32),
            pltpu.VMEM((tile, tile), F32),
            pltpu.VMEM((nodes // blk, blk, tile), F32),
                *[pltpu.VMEM((tile, classes), F32)] * 8,
            *[pltpu.VMEM((tile, tile), F32)] * 8,
            pltpu.VMEM((slots, n), jnp.int32),
            pltpu.VMEM((slots, n), jnp.int32),
            pltpu.VMEM((1, n), jnp.int32),
            pltpu.VMEM((tiles, tile), jnp.int32),
            pltpu.VMEM((n, 1, tile), jnp.int32),
            pltpu.VMEM((n, 1, tile), jnp.int32),
            pltpu.SMEM((n, 1, tile), jnp.int32),
            dma((3,)),
            dma((4,)),
            dma,
            dma,
            dma((n // RUN,)),
            dma((2, 2)),
            dma((2, 2, n // CHUNK)),
            dma,
            dma,
            dma((2, 2)),
            dma((2, 2)),
        ],
        compiler_params=pltpu.CompilerParams(
            collective_id=0, has_side_effects=True, vmem_limit_bytes=52 * 2**20
        ),
    )(
        *(
            pltpu.with_memory_space_constraint(x, pltpu.HBM)
            for x in (
                labels,
                band_w,
                far_w.reshape(n, slots * blk, tile),
                far_block[0].T,
                far_tile[0].T,
                far_count,
                seed_mask.reshape(tiles, tile),
            )
        )
    )
    return pl.pallas_call(
        functools.partial(close, tiles, tile, 32),
        out_shape=(
            jax.ShapeDtypeStruct((nodes, classes), BF),
            jax.ShapeDtypeStruct((2, tiles), F32),
        ),
        in_specs=[vmem] * 3,
        out_specs=(hbm, hbm),
        scratch_shapes=[
            pltpu.VMEM((tiles, 8, tile), F32),
            pltpu.VMEM((2, tiles), F32),
            dma,
            dma,
        ],
        compiler_params=pltpu.CompilerParams(vmem_limit_bytes=4 * 2**20),
    )(*(pltpu.with_memory_space_constraint(x, pltpu.VMEM) for x in (new, old, first)))


def solution(mesh):
    placed = (
        P("node", None),
        P("node"),
        P("node", None, None, None),
        P("node", None, None),
        P("node", None, None),
        P("node", None),
        P("node", None, None, None, None),
    )
    return jax.shard_map(
        body,
        mesh=mesh,
        in_specs=placed,
        out_specs=(P("node", None), P(None, "node")),
        check_vma=False,
    )
```

```python
import functools

import jax
import jax.numpy as jnp
from jax import lax
from jax.experimental import pallas as pl
from jax.experimental.pallas import tpu as pltpu
from jax.sharding import PartitionSpec as P

MESH = pl.DeviceIdType.MESH
BF = jnp.bfloat16
F32 = jnp.float32
STEP = 91
BACK = 83
CHUNK = 16
FLOOR = 0.05
RUN = 8


def rows_of(start, size):
    return pl.ds(pl.multiple_of(start, size), size)


def fold_rows(change):
    rows, classes = change.shape
    total = jnp.sum(change.reshape(rows // 8, 8, classes), axis=0)
    return sum(total[:, i : i + 128] for i in range(0, classes, 128))


def close(tiles, tile, sub, new, old, first, out_hbm, res_hbm, second, res, copy_sem, res_sem):
    copy = pltpu.make_async_copy(new, out_hbm, copy_sem)
    copy.start()

    def change(t, carry):
        total = jnp.zeros((8, tile), F32)
        for j in range(tile // sub):
            low = t * tile + j * sub
            after = new[rows_of(low, sub), :]
            before = old[pl.ds(pl.multiple_of(tile + low, sub), sub), :]
            total = total + fold_rows(jnp.abs(after - before).astype(F32))
        second[t] = total
        return carry

    lax.fori_loop(0, tiles, change, 0)
    for it, part in enumerate((first, second)):
        block = jnp.concatenate([jnp.sum(part[...], axis=1), jnp.zeros((tile - tiles, tile), F32)], axis=0)
        res[it : it + 1, :] = jnp.sum(block.T, axis=0, keepdims=True)[:, :tiles]
    small = pltpu.make_async_copy(res, res_hbm, res_sem)
    small.start()
    small.wait()
    copy.wait()


def kernel(
    n, tiles, tile, classes, slots, blk,
    lab_hbm, bw_hbm, fw_hbm, fb_hbm, ft_hbm, fc_hbm, sm_hbm,
    out_ref, p1, resb,
    p0, g32, acc, halo, send, recv, fsend, frecv, wf, bw, fw, wp, wt, mask, oh, dt, inv, ups, sum0, sum1, sum2, sum3, sum4, sum5, sum6, sum7,
    fac0, fac1, fac2, fac3, fac4, fac5, fac6, fac7,
    fb, ft, fc, sm, req, qv, qs,
    load_sem, small_sem, req_ssem, req_rsem, q_sem, ssem, rsem, f_ssem, f_rsem, h_ssem, h_rsem,
):
    me = lax.axis_index("node")
    nodes = tiles * tile
    pair = slots * blk
    wide = n * pair
    def get(ref, row, size):
        part = pl.ds(pl.multiple_of(row // blk, size // blk), size // blk)
        return ref[part].reshape(size, ref.shape[2])

    def put(ref, row, size, value):
        part = pl.ds(pl.multiple_of(row // blk, size // blk), size // blk)
        ref[part] = value.reshape(size // blk, blk, ref.shape[2])

    sums = (sum0, sum1, sum2, sum3, sum4, sum5, sum6, sum7)
    factors = (fac0, fac1, fac2, fac3, fac4, fac5, fac6, fac7)
    chunks = n // CHUNK
    half = classes // 2
    kdim = CHUNK * pair

    def plus(a, b):
        return (a + b) & (n - 1)

    def source_of(p):
        return plus(me, p * STEP)

    def target_of(p):
        return plus(me, -p * STEP)

    def far_first():
        def hops(s):
            return sum(min(s // d % 4, 4 - s // d % 4) for d in (2, 8, 32))

        return sorted(range(1, n), key=lambda s: (-hops(s), s))

    small = [
        pltpu.make_async_copy(src, dst, small_sem.at[i])
        for i, (src, dst) in enumerate(((fb_hbm, fb), (ft_hbm, ft), (fc_hbm, fc), (sm_hbm, sm)))
    ]
    large = [
        pltpu.make_async_copy(fw_hbm, fw, load_sem.at[0]),
        pltpu.make_async_copy(lab_hbm, p0.at[pl.ds(tile, nodes)], load_sem.at[1]),
        pltpu.make_async_copy(bw_hbm, bw, load_sem.at[2]),
    ]
    for copy in small + large:
        copy.start()
    barrier = pltpu.get_barrier_semaphore()

    with jax.named_scope("s_greet"):
        for distance in far_first():
            pl.semaphore_signal(barrier, inc=1, device_id=(plus(me, distance),), device_id_type=MESH)
    for copy in small:
        copy.wait()

    lane = lax.broadcasted_iota(jnp.int32, (n, tile), 1)
    columns = [jnp.broadcast_to(fb[k : k + 1, :], (n, n)).T for k in range(slots)]
    table = jnp.where(lane == 0, columns[0], columns[1])
    for s in range(n):
        req[s] = table[s : s + 1]

    with jax.named_scope("s_barrier"):
        pl.semaphore_wait(barrier, n - 1)

    with jax.named_scope("s_ask"):
        for distance in far_first():
            s = plus(me, distance)
            pltpu.make_async_remote_copy(
                req.at[s], qv.at[distance * BACK % n], req_ssem, req_rsem, device_id=(s,), device_id_type=MESH
            ).start()
    qv[0] = req[me]
    large[1].wait()

    nxt = plus(me, 1)
    prv = plus(me, n - 1)

    def halo_copies(it, cur, low=0, size=tile):
        part = pl.ds(low, size)
        up = pltpu.make_async_remote_copy(
            cur.at[pl.ds(nodes + low, size)], halo.at[it, 0, part], h_ssem.at[it, 0], h_rsem.at[it, 0],
            device_id=(nxt,), device_id_type=MESH,
        )
        down = pltpu.make_async_remote_copy(
            cur.at[pl.ds(tile + low, size)], halo.at[it, 1, part], h_ssem.at[it, 1], h_rsem.at[it, 1],
            device_id=(prv,), device_id_type=MESH,
        )
        return up, down

    halo0 = halo_copies(0, p0)
    for copy in halo0:
        copy.start()

    def widen(t, carry):
        rows = p0[rows_of(tile + t * tile, tile), :].astype(F32)
        g32[rows_of(t * (tile // blk), tile // blk)] = rows.reshape(tile // blk, blk, classes)
        return carry

    lax.fori_loop(0, tiles, widen, 0)
    edge = jnp.zeros((tile, classes), BF)
    for ref in (p0, p1):
        ref[pl.ds(0, tile), :] = edge
        ref[pl.ds(tile + nodes, tile), :] = edge

    large[0].wait()

    def place(p, carry):
        wp[p] = fw[source_of(p)]
        return carry

    lax.fori_loop(0, n, place, 0)

    def turn(j):
        part = wp[pl.ds(j * (tile // pair), tile // pair)].reshape(tile, tile)
        return part.astype(F32).T.astype(BF)

    def turn_chunk(c, carry):
        wt[c] = jnp.concatenate([turn(c * (kdim // tile) + j) for j in range(kdim // tile)], axis=1)
        return carry

    lax.fori_loop(0, chunks, turn_chunk, 0)

    row8 = lax.broadcasted_iota(jnp.int32, (8, n), 0)
    number = [jnp.where(fc[...] > k, ft[k : k + 1, :], -1) for k in range(slots)]
    numbers = jnp.where(row8 == 0, number[0], number[1]).astype(F32).astype(BF)
    step = 512

    def mark(j, carry):
        col = lax.broadcasted_iota(jnp.int32, (n, step), 1) + j * step
        src = (me + (col // pair) * STEP) & (n - 1)
        pick = jnp.where(lax.broadcasted_iota(jnp.int32, (n, step), 0) == src, 1.0, 0.0).astype(BF)
        found = jnp.dot(numbers, pick, preferred_element_type=F32)
        first = lax.rem(col[:1] // blk, slots) == 0
        mine = jnp.where(first, found[:1], found[1:2])
        ids = lax.broadcasted_iota(jnp.int32, (tiles, step), 0).astype(F32)
        oh[:, rows_of(j * step, step)] = jnp.where(mine == ids, 1.0, 0.0)
        return carry

    lax.fori_loop(0, wide // step, mark, 0)

    far_deg = jnp.dot(oh[...].astype(BF), wp[...].reshape(wide, tile), preferred_element_type=F32)
    seeds = sm[...].astype(F32)
    stack = jnp.concatenate([far_deg, seeds, jnp.zeros((tile - 2 * tiles, tile), F32)], axis=0)
    dt[...] = stack.T
    asked = pltpu.make_async_remote_copy(
        req.at[pl.ds(1, n - 1)], qv.at[pl.ds(1, n - 1)], req_ssem, req_rsem,
        device_id=(nxt,), device_id_type=MESH,
    )
    with jax.named_scope("s_waitreq"):
        asked.wait_recv()
    def to_scalar(g):
        span = pl.ds(g * RUN, RUN)
        return pltpu.make_async_copy(qv.at[span], qs.at[span], q_sem.at[g])

    runs = n // RUN
    for g in range(runs):
        to_scalar(g).start()

    def band(cur, t):
        lhs = jnp.concatenate([bw[t, 0], bw[t, 1], bw[t, 2]], axis=1)
        rhs = cur[pl.ds(pl.multiple_of(t * tile, tile), 3 * tile), :]
        put(acc, t * tile, tile, jnp.dot(lhs, rhs, preferred_element_type=F32))

    def band_all(cur):
        def inner(i, carry):
            for j in range(8):
                band(cur, 8 * i + j)
            return carry

        lax.fori_loop(0, tiles // 8, inner, 0)

    def edges(it, copies):
        for copy in copies:
            copy.wait_recv()
        for side, t, o in ((0, 0, 0), (1, tiles - 1, 2)):
            more = jnp.dot(bw[t, o], halo[it, side], preferred_element_type=F32)
            put(acc, t * tile, tile, get(acc, t * tile, tile) + more)

    def arrived(it, h, c, low=0):
        span = pl.ds(c * CHUNK + low, CHUNK - low)
        pltpu.make_async_remote_copy(
            send.at[it, h, span], recv.at[it, h, span], ssem.at[it, h], rsem.at[it, h, c],
            device_id=(nxt,), device_id_type=MESH,
        ).wait_recv()

    def product(it, h, c, t, count):
        span = pl.ds(c * CHUNK, CHUNK)
        if h is None:
            rhs = jnp.concatenate([recv[it, k, span].reshape(kdim, half) for k in range(2)], axis=1)
        else:
            rhs = recv[it, h, span].reshape(kdim, half)
        weights = (wt if it == 0 else wf)[c].reshape(tile // 16, 16, kdim)
        parts = [(weights * mask[c, t + j][None]).reshape(tile, kdim) for j in range(count)]
        lhs = parts[0] if count == 1 else jnp.concatenate(parts, axis=0)
        return jnp.dot(lhs, rhs, preferred_element_type=F32)

    group = tiles

    def multiply(it, h, c):
        cols = pl.ds(0, classes) if h is None else pl.ds(h * half, half)

        def some(g, inner):
            size = group * tile // blk
            part = pl.ds(pl.multiple_of(g * size, size), size)
            more = product(it, h, c, g * group, group)
            acc[part, :, cols] = acc[part, :, cols] + more.reshape(size, blk, more.shape[1])
            return inner

        with jax.named_scope("s_mm"):
            lax.fori_loop(0, tiles // group, some, 0)

    def far(it, h, count):
        halves = (0, 1) if h is None else (h,)

        def chunk(c, carry):
            with jax.named_scope("s_wait"):
                for k in halves:
                    arrived(it, k, c)
            multiply(it, h, c)
            return carry

        for k in halves:
            arrived(it, k, 0, 1)
        multiply(it, h, jnp.int32(0))
        lax.fori_loop(1, count, chunk, 0)

    sub = 32
    reps = classes // tile

    def lift(spread, one):
        square = jnp.sum(spread * spread, axis=1, keepdims=True)
        mean = square * one * one * (1.0 / classes)
        return lax.rsqrt(jnp.maximum(mean, FLOOR * FLOOR))

    def factor_of(spread, one):
        return one * lift(spread, one)

    def chosen(spread, factor, signed, given):
        reps = spread.shape[1] // tile
        seeded = jnp.concatenate([signed] * reps, axis=1) < 0.0
        return jnp.where(seeded, given, spread * jnp.concatenate([factor] * reps, axis=1))

    def scale(it, t, slot):
        spread = get(acc, t * tile, 2 * tile) + product(it, None, chunks - 1, t, 2)
        factor = factor_of(spread, jnp.abs(get(inv, t * tile, 2 * tile)))
        for k in range(2):
            part = slice(k * tile, (k + 1) * tile)
            sums[slot + k][...] = spread[part]
            factors[slot + k][...] = factor[part]

    def fresh(t, slot, j):
        part = pl.ds(j * sub, sub)
        row = t * tile + j * sub
        given = p0[pl.ds(pl.multiple_of(tile + row, sub), sub), :].astype(F32)
        return chosen(sums[slot][part, :], factors[slot][part, :], get(inv, row, sub), given)

    fold = fold_rows

    def settle(t):
        total = jnp.zeros((8, tile), F32)
        for j in range(tile // sub):
            row = t * tile + j * sub
            rows = pl.ds(pl.multiple_of(tile + row, sub), sub)
            spread, signed = get(acc, row, sub), get(inv, row, sub)
            given = p0[rows, :].astype(F32)
            new = chosen(spread, jnp.abs(signed) * get(ups, row, sub), signed, given).astype(BF)
            p1[rows, :] = new
            total = total + fold(jnp.abs(new.astype(F32) - given))
        resb[t] = total

    def ship(it, h, g, low=0):
        for j in range(low, RUN):
            p = g * RUN + j
            pltpu.make_async_remote_copy(
                send.at[it, h, p], recv.at[it, h, p], ssem.at[it, h], rsem.at[it, h, g // (CHUNK // RUN)],
                device_id=(target_of(p),), device_id_type=MESH,
            ).start()

    def pair_of(block, p):
        return jnp.concatenate([block(qs[p, 0, k]) for k in range(slots)], axis=0).astype(BF)

    zero = jnp.int32(0)

    def exchange_labels():
        def load(g, low=0):
            to_scalar(g).wait()
            for j in range(low, RUN):
                rows = pair_of(lambda b: g32[b], g * RUN + j)
                send[0, 0, g * RUN + j] = rows[:, :half]
                send[0, 1, g * RUN + j] = rows[:, half:]

        def both(g, carry):
            load(g)
            ship(0, 0, g - 1)
            return carry

        def rest(g, carry):
            ship(0, 1, g)
            return carry

        load(zero, 1)
        own = pair_of(lambda b: g32[b], 0)
        recv[0, 0, 0] = own[:, :half]
        recv[0, 1, 0] = own[:, half:]
        load(zero + 1)
        ship(0, 0, zero, 1)
        lax.fori_loop(2, runs, both, 0)
        ship(0, 0, zero + (runs - 1))
        ship(0, 1, zero, 1)
        lax.fori_loop(1, runs, rest, 0)

    def gather_averages(h, g, low=0):
        def block(b):
            signed = inv[b]
            cols = slice(h * half, (h + 1) * half)
            return chosen(acc[b][:, cols], jnp.abs(signed), signed, g32[b][:, cols])

        for j in range(low, RUN):
            send[1, h, g * RUN + j] = pair_of(block, g * RUN + j)
        if isinstance(g, int) and g == 0:
            recv[1, h, 0] = pair_of(block, 0)

    def exchange_averages(h):
        def both(g, carry):
            gather_averages(h, g)
            ship(1, h, g - 1)
            return carry

        def both_and_halo(g, carry):
            low = pl.multiple_of((g - runs // 2) * 16, 16)
            for copy in halo_copies(1, p1, low, 16):
                copy.start()
            return both(g, carry)

        gather_averages(h, 0, 1)
        gather_averages(h, zero + 1)
        ship(1, h, zero, 1)
        lax.fori_loop(2, runs // 2, both, 0)
        if h == 1:
            settle(0)
            settle(tiles - 1)
        lax.fori_loop(runs // 2, runs, both_and_halo if h == 1 else both, 0)
        ship(1, h, zero + (runs - 1))

    def exchange_lifts():
        def load(g, carry):
            lifts = []
            for j in range(RUN):
                for k in range(slots):
                    lifts.append(ups[qs[g * RUN + j, 0, k]])
            fsend[g] = jnp.concatenate(lifts, axis=0).T[:1]
            return carry

        def tell(g, low=0):
            for j in range(low, RUN):
                p = g * RUN + j
                pltpu.make_async_remote_copy(
                    fsend.at[g], frecv.at[p], f_ssem, f_rsem, device_id=(target_of(p),), device_id_type=MESH
                ).start()

        def load_and_tell(g, carry):
            load(g, carry)
            tell(g - 1)
            return carry

        def measure(i, carry):
            for j in range(8):
                row = (8 * i + j) * tile
                signed = get(inv, row, tile)
                put(ups, row, tile, jnp.where(signed < 0.0, 1.0, lift(get(acc, row, tile), jnp.abs(signed))))
            return carry

        with jax.named_scope("s_measure"):
            lax.fori_loop(0, tiles // 8, measure, 0)
        load(zero, 0)
        frecv[0] = fsend[0]
        load(zero + 1, 0)
        tell(zero, 1)
        lax.fori_loop(2, runs, load_and_tell, 0)
        tell(zero + (runs - 1))

    def told():
        pltpu.make_async_remote_copy(
            frecv.at[pl.ds(1, n - 1)], frecv.at[pl.ds(1, n - 1)], f_ssem, f_rsem,
            device_id=(nxt,), device_id_type=MESH,
        ).wait_recv()
        place_of = lax.broadcasted_iota(jnp.int32, (1, tile), 1) // pair

        def apply(c, carry):
            lanes = []
            for i in range(CHUNK // RUN):
                row = jnp.zeros((1, tile), F32)
                for j in range(RUN):
                    row = jnp.where(place_of == j, frecv[c * CHUNK + i * RUN + j], row)
                lanes.append(row)
            wf[c] = (wt[c].astype(F32) * jnp.concatenate(lanes, axis=1)).astype(BF)
            return carry

        lax.fori_loop(0, chunks, apply, 0)

    def finish(it, write):
        def step(i, carry):
            t = 8 * i
            for j in (0, 2):
                scale(it, t + 4 + j, 4 + j)
                write(t + j, j)
                write(t + j + 1, j + 1)
            for j in (0, 2):
                scale(it, t + 8 + j, j)
                write(t + 4 + j, 4 + j)
                write(t + 5 + j, 5 + j)
            return carry

        for j in (0, 2):
            scale(it, jnp.int32(j), j)
        lax.fori_loop(0, tiles // 8 - 1, step, 0)
        t = jnp.int32(tiles - 8)
        for j in (0, 2):
            scale(it, t + 4 + j, 4 + j)
            write(t + j, j)
            write(t + j + 1, j + 1)
        for j in range(4):
            write(t + 4 + j, 4 + j)

    with jax.named_scope("s_exchange0"):
        exchange_labels()

    large[2].wait()

    def invert(i, carry):
        both = dt[...]
        for k in range(4):
            t = i * 4 + k
            far = jnp.sum(jnp.where(lane == t, both, 0.0), axis=1, keepdims=True)
            seed = jnp.sum(jnp.where(lane == t + tiles, both, 0.0), axis=1, keepdims=True)
            weight = bw[t, 0].astype(F32) + bw[t, 1].astype(F32) + bw[t, 2].astype(F32)
            one = 1.0 / (jnp.sum(weight, axis=1, keepdims=True) + far)
            put(inv, t * tile, tile, jnp.broadcast_to(jnp.where(seed > 0.5, -one, one), (tile, tile)))
        return carry

    with jax.named_scope("s_invert"):
        lax.fori_loop(0, tiles // 4, invert, 0)

    def spread_mask(c, carry):
        def some(i, inner):
            rows = oh[rows_of(i * 8, 8), rows_of(c * kdim, kdim)]
            for j in range(8):
                mask[c, i * 8 + j] = jnp.broadcast_to(rows[j : j + 1], (16, kdim)).astype(BF)
            return inner

        lax.fori_loop(0, tiles // 8, some, 0)
        return carry

    with jax.named_scope("s_mask"):
        lax.fori_loop(0, chunks, spread_mask, 0)
    with jax.named_scope("s_band0"):
        band_all(p0)
    far(0, 0, chunks)
    edges(0, halo0)
    with jax.named_scope("s_averages"):
        exchange_averages(0)
    far(0, 1, chunks)

    halo1 = halo_copies(1, p1)
    with jax.named_scope("s_exchange1"):
        exchange_lifts()
        with jax.named_scope("s_second"):
            exchange_averages(1)

    def settle_five(i, carry):
        for j in range(5):
            settle(5 * i + 1 + j)
        return carry

    with jax.named_scope("s_settle"):
        lax.fori_loop(0, (tiles - 2) // 5, settle_five, 0)
    with jax.named_scope("s_band1"):
        band_all(p1)
    with jax.named_scope("s_told"):
        told()
    far(1, 0, chunks - 1)
    far(1, 1, chunks - 1)
    edges(1, halo1)
    with jax.named_scope("s_waitlast"):
        for h in range(2):
            arrived(1, h, chunks - 1)

    def write1(t, slot):
        for j in range(tile // sub):
            out_ref[rows_of(t * tile + j * sub, sub), :] = fresh(t, slot, j).astype(BF)

    with jax.named_scope("s_finish1"):
        finish(1, write1)

    asked.wait_send()
    for copy in halo0 + halo1:
        copy.wait_send()
    span = pl.ds(1, n - 1)
    for it in range(2):
        for h in range(2):
            pltpu.make_async_remote_copy(
                send.at[it, h, span], recv.at[it, h, span], ssem.at[it, h], rsem.at[it, h, 0],
                device_id=(nxt,), device_id_type=MESH,
            ).wait_send()
    pltpu.make_async_remote_copy(
        frecv.at[span], frecv.at[span], f_ssem, f_rsem, device_id=(nxt,), device_id_type=MESH
    ).wait_send()


def body(labels, seed_mask, band_w, far_block, far_tile, far_count, far_w):
    nodes, classes = labels.shape
    tiles, _, tile, _ = band_w.shape
    _, n, slots, blk, _ = far_w.shape
    hbm = pl.BlockSpec(memory_space=pltpu.HBM)
    vmem = pl.BlockSpec(memory_space=pltpu.VMEM)
    dma = pltpu.SemaphoreType.DMA
    wide = n * slots * blk
    new, old, first = pl.pallas_call(
        functools.partial(kernel, n, tiles, tile, classes, slots, blk),
        out_shape=(
            pltpu.VMEM((nodes, classes), BF),
            pltpu.VMEM((nodes + 2 * tile, classes), BF),
            pltpu.VMEM((tiles, 8, tile), F32),
        ),
        in_specs=[hbm] * 7,
        out_specs=(vmem, vmem, vmem),
        scratch_shapes=[
            pltpu.VMEM((nodes + 2 * tile, classes), BF),
            pltpu.VMEM((nodes // blk, blk, classes), F32),
            pltpu.VMEM((nodes // blk, blk, classes), F32),
            pltpu.VMEM((2, 2, tile, classes), BF),
            pltpu.VMEM((2, 2, n, slots * blk, classes // 2), BF),
            pltpu.VMEM((2, 2, n, slots * blk, classes // 2), BF),
            pltpu.VMEM((n // RUN, 1, tile), F32),
            pltpu.VMEM((n, 1, tile), F32),
            pltpu.VMEM((n // CHUNK, tile, CHUNK * slots * blk), BF),
            pltpu.VMEM(band_w.shape, BF),
            pltpu.VMEM((n, slots * blk, tile), BF),
            pltpu.VMEM((n, slots * blk, tile), BF),
            pltpu.VMEM((n // CHUNK, tile, CHUNK * slots * blk), BF),
            pltpu.VMEM((n // CHUNK, tiles, 16, CHUNK * slots * blk), BF),
            pltpu.VMEM((tiles, wide), F32),
            pltpu.VMEM((tile, tile), F32),
            pltpu.VMEM((nodes // blk, blk, tile), F32),
            pltpu.VMEM((nodes // blk, blk, tile), F32),
                *[pltpu.VMEM((tile, classes), F32)] * 8,
            *[pltpu.VMEM((tile, tile), F32)] * 8,
            pltpu.VMEM((slots, n), jnp.int32),
            pltpu.VMEM((slots, n), jnp.int32),
            pltpu.VMEM((1, n), jnp.int32),
            pltpu.VMEM((tiles, tile), jnp.int32),
            pltpu.VMEM((n, 1, tile), jnp.int32),
            pltpu.VMEM((n, 1, tile), jnp.int32),
            pltpu.SMEM((n, 1, tile), jnp.int32),
            dma((3,)),
            dma((4,)),
            dma,
            dma,
            dma((n // RUN,)),
            dma((2, 2)),
            dma((2, 2, n // CHUNK)),
            dma,
            dma,
            dma((2, 2)),
            dma((2, 2)),
        ],
        compiler_params=pltpu.CompilerParams(
            collective_id=0, has_side_effects=True, vmem_limit_bytes=54 * 2**20
        ),
    )(
        *(
            pltpu.with_memory_space_constraint(x, pltpu.HBM)
            for x in (
                labels,
                band_w,
                far_w.reshape(n, slots * blk, tile),
                far_block[0].T,
                far_tile[0].T,
                far_count,
                seed_mask.reshape(tiles, tile),
            )
        )
    )
    return pl.pallas_call(
        functools.partial(close, tiles, tile, 32),
        out_shape=(
            jax.ShapeDtypeStruct((nodes, classes), BF),
            jax.ShapeDtypeStruct((2, tiles), F32),
        ),
        in_specs=[vmem] * 3,
        out_specs=(hbm, hbm),
        scratch_shapes=[
            pltpu.VMEM((tiles, 8, tile), F32),
            pltpu.VMEM((2, tiles), F32),
            dma,
            dma,
        ],
        compiler_params=pltpu.CompilerParams(vmem_limit_bytes=4 * 2**20),
    )(*(pltpu.with_memory_space_constraint(x, pltpu.VMEM) for x in (new, old, first)))


def solution(mesh):
    placed = (
        P("node", None),
        P("node"),
        P("node", None, None, None),
        P("node", None, None),
        P("node", None, None),
        P("node", None),
        P("node", None, None, None, None),
    )
    return jax.shard_map(
        body,
        mesh=mesh,
        in_specs=placed,
        out_specs=(P("node", None), P(None, "node")),
        check_vma=False,
    )
```
